256 devices in a mesh: lb: 8 (over z), rb: 16 (over x, y), wa: 2 (over core).
Axes of the slice: x: 4, y: 4, z: 8, core: 2. Of those that a mesh axis runs over, the one named last changes fastest.
Arguments:
- initial_guess: bfloat16 [8192, 4, 128], P(('lb', 'rb')), may hold values from -6 to 6
- left_environment: bfloat16 [8, 8, 16, 64, 8192], P('wa', None, 'rb', None, 'lb'), may hold values from -12 to 12, as said below
- right_environment: bfloat16 [128, 8, 128], replicated, may hold values from -12 to 12, as said below
- operator_blocks: float32 [16, 4, 4], replicated, may hold values from -4 to 4
- operator_pairs: int32 [16, 2], replicated, may hold values from 0 to 7
Outputs:
- ritz_vector: float32 [8192, 4, 128], P(('lb', 'rb'))
- residual: float32 [8192, 4, 128], P(('lb', 'rb'))
The draws below stay inside these ranges and needn't reach their ends.
Inputs may be any that keep to these rules, and one draw needn't show every extreme that they name: `operator_pairs`: each row names the left and the right MPO index of one operator block; blocks with the same pair add. `left_environment`: for each MPO index the [8192, 8192] matrix is symmetric. `right_environment`: for each MPO index the matrix over the two right bond states is symmetric.
All inputs are finite; a program needn't handle non-finite values.
Results may differ from the reference program's by a relative error of at most 0.014.
Values may be sent and summed in bfloat16 or wider, within the bound.
A program may use at most 128 MiB of HBM per device.

```python
import jax
import jax.numpy as jnp
from jax import lax

DL = 8192
RB = 128
W = 8
NB = 16
ITERS = 3
SWEEPS = 8
S = 4
N_LB = 8
N_RB = 16


def draw_left_environment(key, part):
    noise_key = jax.random.fold_in(key, 11)
    scale_key = jax.random.fold_in(key, 12)
    noise = jax.random.normal(noise_key, (W, DL, DL), jnp.float32)
    symmetric = (noise + jnp.swapaxes(noise, 1, 2)) * (0.5 / jnp.sqrt(DL * 1.0))
    scales = jnp.exp(jax.random.uniform(scale_key, (W, DL), jnp.float32, 0.0, 2.0))
    positions = jnp.arange(DL, dtype=jnp.int32)
    symmetric = symmetric.at[:, positions, positions].add(scales)
    return symmetric.reshape(W, N_LB, N_RB, DL // (N_LB * N_RB), DL).astype(jnp.bfloat16)


def draw_right_environment(key, part):
    noise_key = jax.random.fold_in(key, 21)
    scale_key = jax.random.fold_in(key, 22)
    noise = jax.random.normal(noise_key, (RB, W, RB), jnp.float32)
    symmetric = (noise + jnp.transpose(noise, (2, 1, 0))) * (0.5 / jnp.sqrt(RB * 1.0))
    scales = jnp.exp(jax.random.uniform(scale_key, (W, RB), jnp.float32, 0.0, 2.0))
    symmetric = symmetric + jnp.eye(RB, dtype=jnp.float32)[:, None, :] * scales[None, :, :]
    return symmetric.astype(jnp.bfloat16)


def place_ends(entries, rng, least, top_value):
    shape = entries.shape
    place = [jax.random.randint(jax.random.fold_in(rng, axis), (), 0, shape[axis]) for axis in range(len(shape))]
    entries = entries.at[tuple(place)].set(least)
    longest = shape.index(max(shape))
    place[longest] = (place[longest] + 1) % shape[longest]
    return entries.at[tuple(place)].set(top_value)


def block_scale(key, dims, split, smallest, high):
    loudness, own = 1.0, jax.random.fold_in(key, 6)
    for axis_at, parts in split:
        draws = jnp.exp(jax.random.uniform(jax.random.fold_in(own, axis_at), (parts,), jnp.float32, smallest / len(split), high / len(split)))
        loudness = loudness * jnp.repeat(draws, dims[axis_at] // parts).reshape([-1 if axis == axis_at else 1 for axis in range(len(dims))])
    return loudness


def scatter_about(key, extent, deviation, reach, shards=(), kind=jnp.bfloat16):
    values = deviation * jax.random.normal(key, extent, jnp.float32)
    if shards:
        values = values * block_scale(key, extent, shards, -0.22, 0.18)
    return jnp.clip(values, -reach, reach).astype(kind)


def setup_inputs(seed: int = 0) -> dict:
    key_list = jax.random.split(jax.random.key(seed), 6)
    initial_guess = scatter_about(key_list[0], (DL, S, RB), 1.0, 6.0, ((0, 128),))
    left_environment = draw_left_environment(jax.random.fold_in(key_list[5], 71), 0)
    right_environment = draw_right_environment(jax.random.fold_in(key_list[5], 71), 0)
    operator_blocks = scatter_about(key_list[3], (NB, S, S), 0.3, 4.0, (), jnp.float32)
    operator_pairs = place_ends(jax.random.randint(key_list[4], (NB, 2), 0, W), jax.random.fold_in(key_list[4], 1), 0, W - 1).astype(jnp.int32)
    return dict(initial_guess=initial_guess, left_environment=left_environment, right_environment=right_environment, operator_blocks=operator_blocks, operator_pairs=operator_pairs)


highest = lax.Precision.HIGHEST
epsilon = 1e-06

def lowest_pair(matrix):
    matrix_order = matrix.shape[0]
    vectors = jnp.eye(matrix_order, dtype=jnp.float32)
    for rounds in range(SWEEPS):
        for first_row in range(matrix_order):
            for second_row in range(first_row + 1, matrix_order):
                rotation_angle = 0.5 * jnp.arctan2(2.0 * matrix[first_row, second_row], matrix[second_row, second_row] - matrix[first_row, first_row])
                cosine = jnp.cos(rotation_angle)
                sine_value = jnp.sin(rotation_angle)
                rotation = jnp.eye(matrix_order, dtype=jnp.float32)
                rotation = rotation.at[first_row, first_row].set(cosine).at[second_row, second_row].set(cosine)
                rotation = rotation.at[first_row, second_row].set(sine_value).at[second_row, first_row].set(-sine_value)
                matrix = jnp.dot(rotation.T, jnp.dot(matrix, rotation, precision=highest), precision=highest)
                vectors = jnp.dot(vectors, rotation, precision=highest)
    values = jnp.diagonal(matrix)
    chosen = (jnp.arange(matrix_order, dtype=jnp.int32) == jnp.argmin(values).astype(jnp.int32)).astype(jnp.float32)
    ritz_value = jnp.sum(values * chosen)
    weights = jnp.dot(vectors, chosen, precision=highest)
    weights = jnp.where(weights[0] < 0.0, -weights, weights)
    return (ritz_value, weights)

def dense_operator(operator_blocks, operator_pairs, levels):
    symmetric = 0.5 * (operator_blocks + jnp.swapaxes(operator_blocks, 1, 2))
    indices = jnp.arange(levels, dtype=jnp.int32)
    left_hot = (operator_pairs[:, 0:1] == indices[None, :]).astype(jnp.float32)
    right_hot = (operator_pairs[:, 1:2] == indices[None, :]).astype(jnp.float32)
    return jnp.einsum('nw,nv,nts->wvts', left_hot, right_hot, symmetric, precision=highest)

def contract_right(vector_rows, right_matrix, local_operator):
    row_count, physical, window = vector_rows.shape
    levels = local_operator.shape[1]
    mixed = jnp.dot(vector_rows.reshape(row_count * physical, window), right_matrix, preferred_element_type=jnp.float32)
    mixed = mixed.reshape(row_count, physical, levels, window)
    return jnp.einsum('kvts,nsvb->kntb', local_operator, mixed, precision=highest).astype(jnp.bfloat16)

def combine(members, weights):
    total = weights[0] * members[0]
    for member_index in range(1, len(members)):
        total = total + weights[member_index] * members[member_index]
    return total

def reference(initial_guess, left_environment, right_environment, operator_blocks, operator_pairs):
    total_count = DL * S * RB
    left_matrix = left_environment.reshape(W, DL, DL)
    right_matrix = right_environment.reshape(RB, W * RB)
    operator = dense_operator(operator_blocks, operator_pairs, W)

    def apply_hamiltonian(vector):
        inner_terms = contract_right(vector.astype(jnp.bfloat16), right_matrix, operator)
        flat = inner_terms.reshape(W, DL, S * RB)
        image = jnp.zeros((DL, S * RB), jnp.float32)
        for level in range(W):
            image = image + jnp.dot(left_matrix[level], flat[level], preferred_element_type=jnp.float32)
        return image.reshape(DL, S, RB)

    def mean_product(first_array, second_array):
        return jnp.sum(first_array * second_array) / total_count
    left_diag = jnp.diagonal(left_matrix, axis1=1, axis2=2).astype(jnp.float32)
    operator_diag = jnp.diagonal(operator, axis1=2, axis2=3)
    right_diag = jnp.diagonal(right_environment, axis1=0, axis2=2).astype(jnp.float32)
    diagonal_values = jnp.einsum('ka,kvs,vb->asb', left_diag, operator_diag, right_diag, precision=highest)
    start_vector = initial_guess.astype(jnp.float32)
    basis = [start_vector * lax.rsqrt(mean_product(start_vector, start_vector) + epsilon)]
    images = [apply_hamiltonian(basis[0])]
    subspace = jnp.zeros((ITERS + 1, ITERS + 1), jnp.float32)
    subspace = subspace.at[0, 0].set(mean_product(basis[0], images[0]))
    for step_index in range(ITERS):
        filled = step_index + 1
        ritz_value, weights = lowest_pair(subspace[:filled, :filled])
        ritz_now = combine(basis, weights)
        residual_now = combine(images, weights) - ritz_value * ritz_now
        correction = residual_now / (jnp.abs(diagonal_values - ritz_value) + 1.0)
        correlations = jnp.stack([mean_product(member, correction) for member in basis])
        correction = correction - combine(basis, correlations)
        new_vector = correction * lax.rsqrt(mean_product(correction, correction) + epsilon)
        new_image = apply_hamiltonian(new_vector)
        basis.append(new_vector)
        images.append(new_image)
        row_values = jnp.stack([mean_product(member, new_image) for member in basis])
        subspace = subspace.at[filled, :filled + 1].set(row_values).at[:filled + 1, filled].set(row_values)
    ritz_value, weights = lowest_pair(subspace)
    ritz_vector = combine(basis, weights)
    residual = combine(images, weights) - ritz_value * ritz_vector
    return (ritz_vector, residual)
```

```python
import functools

import jax
import jax.numpy as jnp
from jax import lax
from jax.experimental import pallas as pl
from jax.experimental.pallas import tpu as pltpu
from jax.sharding import PartitionSpec as P

ITERS = 3
SWEEPS = 8
STEPS = ITERS + 1
TILE = (8, 128)
LB_RB = ("lb", "rb")
MESH_ID = pl.DeviceIdType.MESH

highest = lax.Precision.HIGHEST
epsilon = 1e-06


def rotate(matrix, vectors, p, q, order):
    y = 2.0 * matrix[p][q]
    x = matrix[q][q] - matrix[p][p]
    square = x * x + y * y
    usable = square > 0.0
    inverse = lax.rsqrt(jnp.where(usable, square, 1.0))
    half_sum = 0.5 + 0.5 * jnp.abs(x * inverse)
    inverse_large = lax.rsqrt(half_sum)
    large = half_sum * inverse_large
    small = 0.5 * jnp.abs(y * inverse) * inverse_large
    forward = x >= 0.0
    cosine = jnp.where(usable, jnp.where(forward, large, small), 1.0)
    sine = jnp.where(usable, jnp.where(forward, small, large), 0.0)
    sine = jnp.where(y < 0.0, -sine, sine)
    m_pp, m_qq, m_pq = matrix[p][p], matrix[q][q], matrix[p][q]
    cc, ss, cs = cosine * cosine, sine * sine, cosine * sine
    cross = 2.0 * cs * m_pq
    matrix[p][p] = cc * m_pp - cross + ss * m_qq
    matrix[q][q] = ss * m_pp + cross + cc * m_qq
    matrix[p][q] = matrix[q][p] = jnp.zeros_like(m_pq)
    for i in range(order):
        if i != p and i != q:
            a, b = matrix[i][p], matrix[i][q]
            matrix[i][p] = matrix[p][i] = cosine * a - sine * b
            matrix[i][q] = matrix[q][i] = sine * a + cosine * b
        a, b = vectors[i][p], vectors[i][q]
        vectors[i][p] = cosine * a - sine * b
        vectors[i][q] = sine * a + cosine * b


def lowest(entries, order):
    if order == 1:
        return entries[0][0], [jnp.ones(TILE, jnp.float32)]
    scale = jnp.abs(entries[0][0])
    for i in range(order):
        for j in range(i, order):
            scale = jnp.maximum(scale, jnp.abs(entries[i][j]))
    inverse = 1.0 / jnp.where(scale > 0.0, scale, 1.0)
    flat = [entries[i][j] * inverse for i in range(order) for j in range(order)]
    flat += [jnp.full(TILE, 1.0 if i == j else 0.0, jnp.float32) for i in range(order) for j in range(order)]

    def sweep(_, flat):
        matrix = [list(flat[i * order : (i + 1) * order]) for i in range(order)]
        base = order * order
        vectors = [list(flat[base + i * order : base + (i + 1) * order]) for i in range(order)]
        for p in range(order):
            for q in range(p + 1, order):
                rotate(matrix, vectors, p, q, order)
        return tuple(v for row in matrix + vectors for v in row)

    flat = lax.fori_loop(0, 1 if order == 2 else SWEEPS, sweep, tuple(flat))
    matrix = [flat[i * order : (i + 1) * order] for i in range(order)]
    base = order * order
    vectors = [flat[base + i * order : base + (i + 1) * order] for i in range(order)]
    best = matrix[0][0]
    weights = [vectors[i][0] for i in range(order)]
    for j in range(1, order):
        less = matrix[j][j] < best
        best = jnp.where(less, matrix[j][j], best)
        weights = [jnp.where(less, vectors[i][j], weights[i]) for i in range(order)]
    negative = weights[0] < 0.0
    weights = [jnp.where(negative, -w, w) for w in weights]
    return best * scale, weights


def kernel(
    dims,
    guess_ref,
    right_ref,
    op_ref,
    left_hbm,
    vector_ref,
    residual_ref,
    left,
    mixing,
    right_rows,
    right_by_level,
    gathered,
    column,
    inner,
    image,
    pair_out,
    pair_in,
    block_out,
    block_in,
    diag_parts,
    diag_in,
    basis,
    images,
    tile_out,
    tiles_a,
    tile_mid,
    tiles_b,
    left_sem,
    x_send,
    x_recv,
    f_send,
    f_recv,
    z_send,
    z_recv,
    p_send,
    p_recv,
    s_send,
    s_recv,
    a_send,
    a_recv,
    b_send,
    b_recv,
    d_sems,
    o_sems,
):
    n_lb, n_rb, line, rows, states, window, levels, local_levels = dims
    lines = n_rb // line
    chunk = line * rows
    half_width = states * window // 2
    block_rows = n_lb * rows
    scale = 1.0 / (n_lb * n_rb * rows * states * window)
    z = lax.axis_index("lb")
    me = lax.axis_index("rb")
    half = lax.axis_index("wa")
    other = 1 - half
    my_line = lax.div(me, line)
    f32, bf16 = jnp.float32, jnp.bfloat16

    def remote(src, dst, send, recv, peer):
        return pltpu.make_async_remote_copy(
            src_ref=src, dst_ref=dst, send_sem=send, recv_sem=recv, device_id=peer, device_id_type=MESH_ID
        )

    def drain(region, sem):
        pltpu.make_async_copy(region, region, sem).wait()

    def each(count, body):
        def step(i, carry):
            body(i)
            return carry

        lax.fori_loop(0, count, step, 0)

    def left_copy(i):
        w, q = lax.div(i, lines), lax.rem(i, lines)
        return pltpu.make_async_copy(
            left_hbm.at[w, :, pl.ds(pl.multiple_of(q * chunk, chunk), chunk)],
            left.at[q, :, pl.ds(pl.multiple_of(w * chunk, chunk), chunk)],
            left_sem,
        )

    each(local_levels * lines, lambda i: left_copy(i).start())

    barrier = pltpu.get_barrier_semaphore()

    def greet(peer):
        pl.semaphore_signal(barrier, inc=1, device_id=peer, device_id_type=MESH_ID)

    each(n_rb - 1, lambda j: greet({"rb": lax.rem(me + 1 + j, n_rb)}))
    each(n_lb - 1, lambda j: greet({"lb": lax.rem(z + 1 + j, n_lb)}))
    each(n_lb, lambda j: greet({"lb": lax.rem(z + j, n_lb), "wa": other}))

    def own(it):
        return gathered.at[it, half, pl.ds(pl.multiple_of(me * rows, rows), rows)]

    def hand_out(it, part):
        own(it)[...] = part
        column[it, z] = part

    def start_hand_out(it):
        def to_plane(j):
            remote(own(it), own(it), x_send.at[it], x_recv.at[it, my_line], {"rb": lax.rem(me + 1 + j, n_rb)}).start()

        def to_column(j):
            remote(column.at[it, z], column.at[it, z], z_send.at[it], z_recv.at[it], {"lb": lax.rem(z + 1 + j, n_lb)}).start()

        each(n_rb - 1, to_plane)
        each(n_lb - 1, to_column)

    def own_half(ref):
        return jnp.where(half == 0, ref[:, :half_width], ref[:, half_width:])

    first = own_half(guess_ref)
    hand_out(0, first)
    current = first.astype(f32)
    pl.semaphore_wait(barrier, (n_rb - 1) + (n_lb - 1) + n_lb)
    start_hand_out(0)

    right_rows[...] = right_ref[...].astype(f32).reshape(window * levels, window)
    for v in range(levels):
        right_by_level[v] = right_rows[pl.ds(v, window, stride=levels), :]

    def op_at(w, v, t, s):
        return op_ref[((w * levels + v) * states + t) * states + s]

    def mix_level(w):
        for t in range(states):
            for s in range(t, states):
                tile = op_at(w, 0, t, s) * right_by_level[0]
                for v in range(1, levels):
                    tile = tile + op_at(w, v, t, s) * right_by_level[v]
                tile = tile.astype(bf16)
                for a, b in {(t, s), (s, t)}:
                    mixing[w, a // 2, b * window : (b + 1) * window, (a % 2) * window : (a % 2 + 1) * window] = tile

    each(local_levels, mix_level)

    row_at = lax.broadcasted_iota(jnp.int32, (window, window), 0)
    col_at = lax.broadcasted_iota(jnp.int32, (window, window), 1)
    right_diag = [
        jnp.sum(jnp.where(row_at == col_at, right_by_level[v], 0.0), axis=0, keepdims=True) for v in range(levels)
    ]
    each(local_levels * lines, lambda i: left_copy(i).wait())
    q_own = my_line
    inside = lax.rem(me, line) * rows
    at_row = lax.broadcasted_iota(jnp.int32, (rows, chunk), 0)
    at_col = lax.broadcasted_iota(jnp.int32, (rows, chunk), 1)
    picked = at_col == at_row + inside
    parts = [jnp.zeros((rows, window), f32) for _ in range(states)]
    for w in range(local_levels):
        entries = left[q_own, pl.ds(pl.multiple_of(z * rows, rows), rows), w * chunk : (w + 1) * chunk].astype(f32)
        left_diag = jnp.sum(jnp.where(picked, entries, 0.0), axis=1, keepdims=True)
        for s in range(states):
            along = op_at(w, 0, s, s) * right_diag[0]
            for v in range(1, levels):
                along = along + op_at(w, v, s, s) * right_diag[v]
            parts[s] = parts[s] + left_diag * along
    for s in range(states):
        diag_parts[s // 2, :, (s % 2) * window : (s % 2 + 1) * window] = parts[s]
    diag_copy = remote(diag_parts.at[other], diag_in, d_sems.at[0], d_sems.at[1], {"wa": other})
    diag_copy.start()

    def spread(number):
        piece = jnp.broadcast_to(number[0:1, :], (rows, TILE[1]))
        return jnp.concatenate([piece] * (half_width // TILE[1]), axis=1)

    def lane_sums(value):
        total = jnp.sum(value, axis=0, keepdims=True)
        out = total[:, : TILE[1]]
        for i in range(1, half_width // TILE[1]):
            out = out + total[:, i * TILE[1] : (i + 1) * TILE[1]]
        return out

    def chunk_rows(q):
        return pl.ds(pl.multiple_of(q * chunk, chunk), chunk)

    def line_at(i):
        if lines == 4:
            i = i + lax.div(i, 2) - 2 * lax.div(i, 3)
        return lax.rem(my_line + i, lines)

    def forward(it, q):
        region = gathered.at[it, half, chunk_rows(q)]
        return remote(region, region, f_send.at[it, q], f_recv.at[it, q], {"wa": other})

    def multiply(it, q):
        x = jnp.concatenate([gathered[it, 0, chunk_rows(q), :], gathered[it, 1, chunk_rows(q), :]], axis=1)

        def to_inner(i):
            h, w = lax.div(i, local_levels), lax.rem(i, local_levels)
            inner[h, chunk_rows(w), :] = jnp.dot(x, mixing[w, h], preferred_element_type=f32).astype(bf16)

        each(2 * local_levels, to_inner)

        def to_image(h):
            image[h] += jnp.dot(left[q], inner[h], preferred_element_type=f32)

        each(2, to_image)

    def apply(it, member):
        image[...] = jnp.zeros_like(image)
        drain(gathered.at[it, half, pl.ds(0, chunk - rows)], x_recv.at[it, my_line])
        forward(it, my_line).start()

        def one_line(i):
            @pl.when(i < lines - 1)
            def _():
                q = line_at(i + 1)
                drain(gathered.at[it, half, chunk_rows(q)], x_recv.at[it, q])
                forward(it, q).start()

            q = line_at(i)
            drain(gathered.at[it, other, chunk_rows(q)], f_recv.at[it, q])
            multiply(it, q)

        each(lines, one_line)

        pair_out[it] = image[other].astype(bf16)
        pair = remote(pair_out.at[it], pair_in.at[it], p_send.at[it], p_recv.at[it], {"wa": other})
        pair.start()
        drain(column.at[it, pl.ds(0, n_lb - 1)], z_recv.at[it])
        sums = [lane_sums(member * member)]
        sums += [lane_sums(basis[j] * member) for j in range(it)]
        sums += [lane_sums(images[j] * member) for j in range(it)]
        pair.wait_recv()
        product = jnp.zeros((1, TILE[1]), f32)
        mine = None
        for b in range(n_lb):
            summed = image[half, b * rows : (b + 1) * rows, :] + pair_in[it, b * rows : (b + 1) * rows, :].astype(f32)
            image[half, b * rows : (b + 1) * rows, :] = summed
            block_out[it, b] = summed.astype(bf16)
            product = product + lane_sums(summed * column[it, b].astype(f32))

        def to_block(j):
            b = lax.rem(z + 1 + j, n_lb)
            remote(block_out.at[it, b], block_in.at[it, z], s_send.at[it], s_recv.at[it], {"lb": b}).start()

        each(n_lb - 1, to_block)

        row = lax.broadcasted_iota(jnp.int32, TILE, 0)
        tile = jnp.zeros(TILE, f32)
        for i, value in enumerate([product] + sums):
            tile = jnp.where(row == i, jnp.broadcast_to(value, TILE), tile)
        totals = add_up(it, tile)

        drain(block_in.at[it, pl.ds(0, n_lb - 1)], s_recv.at[it])
        total = image[half, pl.ds(pl.multiple_of(z * rows, rows), rows), :]
        for j in range(1, n_lb):
            total = total + block_in[it, lax.rem(z + j, n_lb)].astype(f32)
        return total, totals

    def add_up(it, tile):
        slot = z * 2 + half
        tiles_a[it, slot] = tile
        tile_out[it] = tile

        def along(j):
            remote(tile_out.at[it], tiles_a.at[it, slot], a_send.at[it], a_recv.at[it], {"lb": lax.rem(z + 1 + j, n_lb)}).start()

        def across(j):
            remote(
                tile_out.at[it], tiles_a.at[it, slot], a_send.at[it], a_recv.at[it],
                {"lb": lax.rem(z + j, n_lb), "wa": other},
            ).start()

        each(n_lb - 1, along)
        each(n_lb, across)
        drain(tiles_a.at[it, pl.ds(0, 2 * n_lb - 1)], a_recv.at[it])
        tile = tiles_a[it, 0]
        for j in range(1, 2 * n_lb):
            tile = tile + tiles_a[it, j]
        tiles_b[it, me] = tile
        tile_mid[it] = tile

        def plane(j):
            remote(tile_mid.at[it], tiles_b.at[it, me], b_send.at[it], b_recv.at[it], {"rb": lax.rem(me + 1 + j, n_rb)}).start()

        each(n_rb - 1, plane)
        drain(tiles_b.at[it, pl.ds(0, n_rb - 1)], b_recv.at[it])
        tile = tiles_b[it, 0]
        for j in range(1, n_rb):
            tile = tile + tiles_b[it, j]
        tile = jnp.broadcast_to(jnp.sum(tile, axis=1, keepdims=True), TILE) * scale
        return [jnp.broadcast_to(tile[i : i + 1, :], TILE) for i in range(2 + 2 * it)]

    entries = [[None] * STEPS for _ in range(STEPS)]
    diagonal = None
    for it in range(STEPS):
        applied, totals = apply(it, current)
        energy, square = totals[0], totals[1]
        overlaps, crossed = totals[2 : 2 + it], totals[2 + it :]
        norm = square
        for a in overlaps:
            norm = norm - a * a
        inverse = lax.rsqrt(jnp.maximum(norm, 0.0) + epsilon)
        for j in range(it):
            value = crossed[j]
            for i in range(it):
                value = value - overlaps[i] * entries[i][j]
            entries[j][it] = entries[it][j] = inverse * value
            energy = energy - overlaps[j] * (crossed[j] + value)
        entries[it][it] = inverse * inverse * energy
        theta, weights = lowest(entries, it + 1)

        vector, applied_now = current, applied
        for j in range(it):
            a = spread(overlaps[j])
            vector = vector - a * basis[j]
            applied_now = applied_now - a * images[j]
        grow = spread(inverse)
        vector, applied_now = vector * grow, applied_now * grow
        basis[it] = vector
        images[it] = applied_now
        last = spread(weights[it])
        ritz, residual = last * vector, last * applied_now
        for j in range(it):
            a = spread(weights[j])
            ritz = ritz + a * basis[j]
            residual = residual + a * images[j]
        shift = spread(theta)
        residual = residual - shift * ritz
        if it == 0:
            diag_copy.wait()
            diagonal = diag_parts[half] + diag_in[...]
            diag_parts[half] = diagonal
        if it < ITERS:
            current = residual / (jnp.abs(diag_parts[half] - shift) + 1.0)
            hand_out(it + 1, current.astype(bf16))
            start_hand_out(it + 1)

    vector_ref[half] = ritz
    residual_ref[half] = residual
    copies = [
        remote(ref.at[half], ref.at[half], o_sems.at[2 * i], o_sems.at[2 * i + 1], {"wa": other})
        for i, ref in enumerate((vector_ref, residual_ref))
    ]
    for copy in copies:
        copy.start()

    def finish(it):
        drain(gathered.at[it, 0, pl.ds(0, (n_rb - 1) * rows)], x_send.at[it])
        drain(column.at[it, pl.ds(0, n_lb - 1)], z_send.at[it])
        each(lines, lambda q: forward(it, q).wait_send())
        drain(pair_out.at[it], p_send.at[it])
        drain(block_out.at[it, pl.ds(0, n_lb - 1)], s_send.at[it])
        drain(tiles_a.at[it, pl.ds(0, 2 * n_lb - 1)], a_send.at[it])
        drain(tiles_b.at[it, pl.ds(0, n_rb - 1)], b_send.at[it])

    each(STEPS, finish)
    for copy in copies:
        copy.wait()


def dense_operator(operator_blocks, operator_pairs, first_level, local_levels, levels):
    symmetric = 0.5 * (operator_blocks + jnp.swapaxes(operator_blocks, 1, 2))
    count = symmetric.shape[0]
    left_hot = operator_pairs[:, 0][:, None] == first_level + jnp.arange(local_levels, dtype=jnp.int32)[None]
    right_hot = operator_pairs[:, 1][:, None] == jnp.arange(levels, dtype=jnp.int32)[None]
    hot = left_hot[:, :, None, None] & right_hot[:, None, :, None]
    return jnp.sum(jnp.where(hot, symmetric.reshape(count, 1, 1, -1), 0.0), axis=0).reshape(-1)


def per_device(initial_guess, left_environment, right_environment, operator_blocks, operator_pairs):
    rows, states, window = initial_guess.shape
    levels = right_environment.shape[1]
    local_levels, n_lb = left_environment.shape[:2]
    contracted = left_environment.shape[4]
    n_rb = lax.axis_size("rb")
    line = 4 if n_rb == 16 else 2
    lines, chunk = n_rb // line, line * rows
    width, half_width = states * window, states * window // 2
    block_rows = n_lb * rows
    operator = dense_operator(
        operator_blocks, operator_pairs, lax.axis_index("wa") * local_levels, local_levels, levels
    )
    dims = (n_lb, n_rb, line, rows, states, window, levels, local_levels)
    f32, bf16 = jnp.float32, jnp.bfloat16
    dma = pltpu.SemaphoreType.DMA
    vmem = pl.BlockSpec(memory_space=pltpu.VMEM)
    out = jax.ShapeDtypeStruct((2, rows, half_width), f32)
    outs = pl.pallas_call(
        functools.partial(kernel, dims),
        out_shape=(out, out),
        in_specs=[vmem, vmem, pl.BlockSpec(memory_space=pltpu.SMEM), pl.BlockSpec(memory_space=pl.ANY)],
        out_specs=(vmem, vmem),
        scratch_shapes=[
            pltpu.VMEM((lines, block_rows, local_levels * chunk), bf16),
            pltpu.VMEM((local_levels, 2, width, half_width), bf16),
            pltpu.VMEM((window * levels, window), f32),
            pltpu.VMEM((levels, window, window), f32),
            pltpu.VMEM((STEPS, 2, contracted, half_width), bf16),
            pltpu.VMEM((STEPS, n_lb, rows, half_width), bf16),
            pltpu.VMEM((2, local_levels * chunk, half_width), bf16),
            pltpu.VMEM((2, block_rows, half_width), f32),
            pltpu.VMEM((STEPS, block_rows, half_width), bf16),
            pltpu.VMEM((STEPS, block_rows, half_width), bf16),
            pltpu.VMEM((STEPS, n_lb, rows, half_width), bf16),
            pltpu.VMEM((STEPS, n_lb, rows, half_width), bf16),
            pltpu.VMEM((2, rows, half_width), f32),
            pltpu.VMEM((rows, half_width), f32),
            pltpu.VMEM((STEPS, rows, half_width), f32),
            pltpu.VMEM((STEPS, rows, half_width), f32),
            pltpu.VMEM((STEPS, *TILE), f32),
            pltpu.VMEM((STEPS, 2 * n_lb, *TILE), f32),
            pltpu.VMEM((STEPS, *TILE), f32),
            pltpu.VMEM((STEPS, n_rb, *TILE), f32),
            dma(()),
            dma((STEPS,)),
            dma((STEPS, lines)),
            dma((STEPS, lines)),
            dma((STEPS, lines)),
            dma((STEPS,)),
            dma((STEPS,)),
            dma((STEPS,)),
            dma((STEPS,)),
            dma((STEPS,)),
            dma((STEPS,)),
            dma((STEPS,)),
            dma((STEPS,)),
            dma((STEPS,)),
            dma((STEPS,)),
            dma((2,)),
            dma((4,)),
        ],
        compiler_params=pltpu.CompilerParams(collective_id=0, has_side_effects=True),
        name="davidson",
    )(
        initial_guess.reshape(rows, width),
        right_environment,
        operator,
        left_environment.reshape(local_levels, block_rows, contracted),
    )
    return tuple(
        o.reshape(2, rows, states // 2, window).transpose(1, 0, 2, 3).reshape(rows, states, window) for o in outs
    )


def solution(mesh):
    in_specs = (P(LB_RB, None, None), P("wa", None, "rb", None, "lb"), P(), P(), P())
    out_specs = (P(LB_RB, None, None), P(LB_RB, None, None))
    return jax.shard_map(per_device, mesh=mesh, in_specs=in_specs, out_specs=out_specs, check_vma=False)
```

```python
import functools

import jax
import jax.numpy as jnp
from jax import lax
from jax.experimental import pallas as pl
from jax.experimental.pallas import tpu as pltpu
from jax.sharding import PartitionSpec as P

ITERS = 3
SWEEPS = 8
STEPS = ITERS + 1
TILE = (8, 128)
LB_RB = ("lb", "rb")
MESH_ID = pl.DeviceIdType.MESH

highest = lax.Precision.HIGHEST
epsilon = 1e-06


def rotate(matrix, vectors, p, q, order):
    y = 2.0 * matrix[p][q]
    x = matrix[q][q] - matrix[p][p]
    square = x * x + y * y
    usable = square > 0.0
    inverse = lax.rsqrt(jnp.where(usable, square, 1.0))
    half_sum = 0.5 + 0.5 * jnp.abs(x * inverse)
    inverse_large = lax.rsqrt(half_sum)
    large = half_sum * inverse_large
    small = 0.5 * jnp.abs(y * inverse) * inverse_large
    forward = x >= 0.0
    cosine = jnp.where(usable, jnp.where(forward, large, small), 1.0)
    sine = jnp.where(usable, jnp.where(forward, small, large), 0.0)
    sine = jnp.where(y < 0.0, -sine, sine)
    m_pp, m_qq, m_pq = matrix[p][p], matrix[q][q], matrix[p][q]
    cc, ss, cs = cosine * cosine, sine * sine, cosine * sine
    cross = 2.0 * cs * m_pq
    matrix[p][p] = cc * m_pp - cross + ss * m_qq
    matrix[q][q] = ss * m_pp + cross + cc * m_qq
    matrix[p][q] = matrix[q][p] = jnp.zeros_like(m_pq)
    for i in range(order):
        if i != p and i != q:
            a, b = matrix[i][p], matrix[i][q]
            matrix[i][p] = matrix[p][i] = cosine * a - sine * b
            matrix[i][q] = matrix[q][i] = sine * a + cosine * b
        a, b = vectors[i][p], vectors[i][q]
        vectors[i][p] = cosine * a - sine * b
        vectors[i][q] = sine * a + cosine * b


def lowest(entries, order):
    if order == 1:
        return entries[0][0], [jnp.ones(TILE, jnp.float32)]
    scale = jnp.abs(entries[0][0])
    for i in range(order):
        for j in range(i, order):
            scale = jnp.maximum(scale, jnp.abs(entries[i][j]))
    inverse = 1.0 / jnp.where(scale > 0.0, scale, 1.0)
    flat = [entries[i][j] * inverse for i in range(order) for j in range(order)]
    flat += [jnp.full(TILE, 1.0 if i == j else 0.0, jnp.float32) for i in range(order) for j in range(order)]

    def sweep(_, flat):
        matrix = [list(flat[i * order : (i + 1) * order]) for i in range(order)]
        base = order * order
        vectors = [list(flat[base + i * order : base + (i + 1) * order]) for i in range(order)]
        for p in range(order):
            for q in range(p + 1, order):
                rotate(matrix, vectors, p, q, order)
        return tuple(v for row in matrix + vectors for v in row)

    flat = lax.fori_loop(0, 1 if order == 2 else SWEEPS, sweep, tuple(flat))
    matrix = [flat[i * order : (i + 1) * order] for i in range(order)]
    base = order * order
    vectors = [flat[base + i * order : base + (i + 1) * order] for i in range(order)]
    best = matrix[0][0]
    weights = [vectors[i][0] for i in range(order)]
    for j in range(1, order):
        less = matrix[j][j] < best
        best = jnp.where(less, matrix[j][j], best)
        weights = [jnp.where(less, vectors[i][j], weights[i]) for i in range(order)]
    negative = weights[0] < 0.0
    weights = [jnp.where(negative, -w, w) for w in weights]
    return best * scale, weights


def kernel(
    dims,
    guess_ref,
    right_ref,
    op_ref,
    left_hbm,
    vector_ref,
    residual_ref,
    left,
    mixing,
    right_rows,
    right_by_level,
    gathered,
    column,
    inner,
    image,
    pair_out,
    pair_in,
    block_out,
    block_in,
    diag_parts,
    diag_in,
    basis,
    images,
    tile_out,
    tiles_a,
    tile_mid,
    tiles_b,
    left_sem,
    x_send,
    x_recv,
    f_send,
    f_recv,
    z_send,
    z_recv,
    p_send,
    p_recv,
    s_send,
    s_recv,
    a_send,
    a_recv,
    b_send,
    b_recv,
    d_sems,
    o_sems,
):
    n_lb, n_rb, line, rows, states, window, levels, local_levels = dims
    lines = n_rb // line
    chunk = line * rows
    half_width = states * window // 2
    block_rows = n_lb * rows
    scale = 1.0 / (n_lb * n_rb * rows * states * window)
    z = lax.axis_index("lb")
    me = lax.axis_index("rb")
    half = lax.axis_index("wa")
    other = 1 - half
    my_line = lax.div(me, line)
    f32, bf16 = jnp.float32, jnp.bfloat16

    def remote(src, dst, send, recv, peer):
        return pltpu.make_async_remote_copy(
            src_ref=src, dst_ref=dst, send_sem=send, recv_sem=recv, device_id=peer, device_id_type=MESH_ID
        )

    def drain(region, sem):
        pltpu.make_async_copy(region, region, sem).wait()

    def each(count, body):
        def step(i, carry):
            body(i)
            return carry

        lax.fori_loop(0, count, step, 0)

    def left_copy(i):
        w, q = lax.div(i, lines), lax.rem(i, lines)
        return pltpu.make_async_copy(
            left_hbm.at[w, :, pl.ds(pl.multiple_of(q * chunk, chunk), chunk)],
            left.at[q, :, pl.ds(pl.multiple_of(w * chunk, chunk), chunk)],
            left_sem,
        )

    each(local_levels * lines, lambda i: left_copy(i).start())

    barrier = pltpu.get_barrier_semaphore()

    def greet(peer):
        pl.semaphore_signal(barrier, inc=1, device_id=peer, device_id_type=MESH_ID)

    each(n_rb - 1, lambda j: greet({"rb": lax.rem(me + 1 + j, n_rb)}))
    each(n_lb - 1, lambda j: greet({"lb": lax.rem(z + 1 + j, n_lb)}))
    each(n_lb, lambda j: greet({"lb": lax.rem(z + j, n_lb), "wa": other}))

    def own(it):
        return gathered.at[it, half, pl.ds(pl.multiple_of(me * rows, rows), rows)]

    def hand_out(it, part):
        own(it)[...] = part
        column[it, z] = part

    def start_hand_out(it):
        def to_plane(j):
            j = j + 1
            away, across = lax.div(j, line), lax.rem(me + j, line)
            if lines == 4:
                away = 4 * lax.div(away + 3, 4) - (away + lax.div(away, 2) - 2 * lax.div(away, 3))
            else:
                away = lines * lax.div(away + lines - 1, lines) - away
            peer = lax.rem(my_line + away, lines) * line + across
            remote(own(it), own(it), x_send.at[it], x_recv.at[it, my_line], {"rb": peer}).start()

        def to_column(j):
            remote(column.at[it, z], column.at[it, z], z_send.at[it], z_recv.at[it], {"lb": lax.rem(z + 1 + j, n_lb)}).start()

        each(n_rb - 1, to_plane)
        each(n_lb - 1, to_column)

    def own_half(ref):
        return jnp.where(half == 0, ref[:, :half_width], ref[:, half_width:])

    first = own_half(guess_ref)
    hand_out(0, first)
    current = first.astype(f32)
    pl.semaphore_wait(barrier, (n_rb - 1) + (n_lb - 1) + n_lb)
    start_hand_out(0)

    right_rows[...] = right_ref[...].astype(f32).reshape(window * levels, window)
    for v in range(levels):
        right_by_level[v] = right_rows[pl.ds(v, window, stride=levels), :]

    def op_at(w, v, t, s):
        return op_ref[((w * levels + v) * states + t) * states + s]

    def mix_level(w):
        for t in range(states):
            for s in range(t, states):
                tile = op_at(w, 0, t, s) * right_by_level[0]
                for v in range(1, levels):
                    tile = tile + op_at(w, v, t, s) * right_by_level[v]
                tile = tile.astype(bf16)
                for a, b in {(t, s), (s, t)}:
                    mixing[w, a // 2, b * window : (b + 1) * window, (a % 2) * window : (a % 2 + 1) * window] = tile

    each(local_levels, mix_level)

    row_at = lax.broadcasted_iota(jnp.int32, (window, window), 0)
    col_at = lax.broadcasted_iota(jnp.int32, (window, window), 1)
    right_diag = [
        jnp.sum(jnp.where(row_at == col_at, right_by_level[v], 0.0), axis=0, keepdims=True) for v in range(levels)
    ]
    each(local_levels * lines, lambda i: left_copy(i).wait())
    q_own = my_line
    inside = lax.rem(me, line) * rows
    at_row = lax.broadcasted_iota(jnp.int32, (rows, chunk), 0)
    at_col = lax.broadcasted_iota(jnp.int32, (rows, chunk), 1)
    picked = at_col == at_row + inside
    parts = [jnp.zeros((rows, window), f32) for _ in range(states)]
    for w in range(local_levels):
        entries = left[q_own, pl.ds(pl.multiple_of(z * rows, rows), rows), w * chunk : (w + 1) * chunk].astype(f32)
        left_diag = jnp.sum(jnp.where(picked, entries, 0.0), axis=1, keepdims=True)
        for s in range(states):
            along = op_at(w, 0, s, s) * right_diag[0]
            for v in range(1, levels):
                along = along + op_at(w, v, s, s) * right_diag[v]
            parts[s] = parts[s] + left_diag * along
    for s in range(states):
        diag_parts[s // 2, :, (s % 2) * window : (s % 2 + 1) * window] = parts[s]
    diag_copy = remote(diag_parts.at[other], diag_in, d_sems.at[0], d_sems.at[1], {"wa": other})
    diag_copy.start()

    def spread(number):
        piece = jnp.broadcast_to(number[0:1, :], (rows, TILE[1]))
        return jnp.concatenate([piece] * (half_width // TILE[1]), axis=1)

    def lane_sums(value):
        total = jnp.sum(value, axis=0, keepdims=True)
        out = total[:, : TILE[1]]
        for i in range(1, half_width // TILE[1]):
            out = out + total[:, i * TILE[1] : (i + 1) * TILE[1]]
        return out

    def chunk_rows(q):
        return pl.ds(pl.multiple_of(q * chunk, chunk), chunk)

    def line_at(i):
        if lines == 4:
            i = i + lax.div(i, 2) - 2 * lax.div(i, 3)
        return lax.rem(my_line + i, lines)

    def forward(it, q):
        region = gathered.at[it, half, chunk_rows(q)]
        return remote(region, region, f_send.at[it, q], f_recv.at[it, q], {"wa": other})

    def multiply(it, q):
        x = jnp.concatenate([gathered[it, 0, chunk_rows(q), :], gathered[it, 1, chunk_rows(q), :]], axis=1)

        for h in range(2):
            for w in range(local_levels):
                inner[h, w * chunk : (w + 1) * chunk, :] = jnp.dot(
                    x, mixing[w, h], preferred_element_type=f32
                ).astype(bf16)
        for h in range(2):
            image[h] += jnp.dot(left[q], inner[h], preferred_element_type=f32)

    def apply(it, member):
        image[...] = jnp.zeros_like(image)
        drain(gathered.at[it, half, pl.ds(0, chunk - rows)], x_recv.at[it, my_line])
        forward(it, my_line).start()

        def one_line(i):
            @pl.when(i < lines - 1)
            def _():
                q = line_at(i + 1)
                drain(gathered.at[it, half, chunk_rows(q)], x_recv.at[it, q])
                forward(it, q).start()

            q = line_at(i)
            drain(gathered.at[it, other, chunk_rows(q)], f_recv.at[it, q])
            multiply(it, q)

        each(lines, one_line)

        pair_out[it] = image[other].astype(bf16)
        pair = remote(pair_out.at[it], pair_in.at[it], p_send.at[it], p_recv.at[it], {"wa": other})
        pair.start()
        drain(column.at[it, pl.ds(0, n_lb - 1)], z_recv.at[it])
        sums = [lane_sums(member * member)]
        sums += [lane_sums(basis[j] * member) for j in range(it)]
        sums += [lane_sums(images[j] * member) for j in range(it)]
        pair.wait_recv()
        product = jnp.zeros((1, TILE[1]), f32)
        mine = None
        for b in range(n_lb):
            summed = image[half, b * rows : (b + 1) * rows, :] + pair_in[it, b * rows : (b + 1) * rows, :].astype(f32)
            image[half, b * rows : (b + 1) * rows, :] = summed
            block_out[it, b] = summed.astype(bf16)
            product = product + lane_sums(summed * column[it, b].astype(f32))

        def to_block(j):
            b = lax.rem(z + 1 + j, n_lb)
            remote(block_out.at[it, b], block_in.at[it, z], s_send.at[it], s_recv.at[it], {"lb": b}).start()

        row = lax.broadcasted_iota(jnp.int32, TILE, 0)
        tile = jnp.zeros(TILE, f32)
        for i, value in enumerate([product] + sums):
            tile = jnp.where(row == i, jnp.broadcast_to(value, TILE), tile)
        totals = add_up(it, tile, lambda: each(n_lb - 1, to_block))

        drain(block_in.at[it, pl.ds(0, n_lb - 1)], s_recv.at[it])
        total = image[half, pl.ds(pl.multiple_of(z * rows, rows), rows), :]
        for j in range(1, n_lb):
            total = total + block_in[it, lax.rem(z + j, n_lb)].astype(f32)
        return total, totals

    def add_up(it, tile, between):
        slot = z * 2 + half
        tiles_a[it, slot] = tile
        tile_out[it] = tile

        def along(j):
            remote(tile_out.at[it], tiles_a.at[it, slot], a_send.at[it], a_recv.at[it], {"lb": lax.rem(z + 1 + j, n_lb)}).start()

        def across(j):
            remote(
                tile_out.at[it], tiles_a.at[it, slot], a_send.at[it], a_recv.at[it],
                {"lb": lax.rem(z + j, n_lb), "wa": other},
            ).start()

        each(n_lb - 1, along)
        each(n_lb, across)
        between()
        drain(tiles_a.at[it, pl.ds(0, 2 * n_lb - 1)], a_recv.at[it])
        tile = tiles_a[it, 0]
        for j in range(1, 2 * n_lb):
            tile = tile + tiles_a[it, j]
        tiles_b[it, me] = tile
        tile_mid[it] = tile

        def plane(j):
            remote(tile_mid.at[it], tiles_b.at[it, me], b_send.at[it], b_recv.at[it], {"rb": lax.rem(me + 1 + j, n_rb)}).start()

        each(n_rb - 1, plane)
        drain(tiles_b.at[it, pl.ds(0, n_rb - 1)], b_recv.at[it])
        tile = tiles_b[it, 0]
        for j in range(1, n_rb):
            tile = tile + tiles_b[it, j]
        tile = jnp.broadcast_to(jnp.sum(tile, axis=1, keepdims=True), TILE) * scale
        return [jnp.broadcast_to(tile[i : i + 1, :], TILE) for i in range(2 + 2 * it)]

    entries = [[None] * STEPS for _ in range(STEPS)]
    diagonal = None
    for it in range(STEPS):
        applied, totals = apply(it, current)
        energy, square = totals[0], totals[1]
        overlaps, crossed = totals[2 : 2 + it], totals[2 + it :]
        norm = square
        for a in overlaps:
            norm = norm - a * a
        inverse = lax.rsqrt(jnp.maximum(norm, 0.0) + epsilon)
        for j in range(it):
            value = crossed[j]
            for i in range(it):
                value = value - overlaps[i] * entries[i][j]
            entries[j][it] = entries[it][j] = inverse * value
            energy = energy - overlaps[j] * (crossed[j] + value)
        entries[it][it] = inverse * inverse * energy
        theta, weights = lowest(entries, it + 1)

        vector, applied_now = current, applied
        for j in range(it):
            a = spread(overlaps[j])
            vector = vector - a * basis[j]
            applied_now = applied_now - a * images[j]
        grow = spread(inverse)
        vector, applied_now = vector * grow, applied_now * grow
        basis[it] = vector
        images[it] = applied_now
        last = spread(weights[it])
        ritz, residual = last * vector, last * applied_now
        for j in range(it):
            a = spread(weights[j])
            ritz = ritz + a * basis[j]
            residual = residual + a * images[j]
        shift = spread(theta)
        residual = residual - shift * ritz
        if it == 0:
            diag_copy.wait()
            diagonal = diag_parts[half] + diag_in[...]
            diag_parts[half] = diagonal
        if it < ITERS:
            current = residual / (jnp.abs(diag_parts[half] - shift) + 1.0)
            hand_out(it + 1, current.astype(bf16))
            start_hand_out(it + 1)

    vector_ref[half] = ritz
    residual_ref[half] = residual
    copies = [
        remote(ref.at[half], ref.at[half], o_sems.at[2 * i], o_sems.at[2 * i + 1], {"wa": other})
        for i, ref in enumerate((vector_ref, residual_ref))
    ]
    for copy in copies:
        copy.start()

    def finish(it):
        drain(gathered.at[it, 0, pl.ds(0, (n_rb - 1) * rows)], x_send.at[it])
        drain(column.at[it, pl.ds(0, n_lb - 1)], z_send.at[it])
        each(lines, lambda q: forward(it, q).wait_send())
        drain(pair_out.at[it], p_send.at[it])
        drain(block_out.at[it, pl.ds(0, n_lb - 1)], s_send.at[it])
        drain(tiles_a.at[it, pl.ds(0, 2 * n_lb - 1)], a_send.at[it])
        drain(tiles_b.at[it, pl.ds(0, n_rb - 1)], b_send.at[it])

    each(STEPS, finish)
    for copy in copies:
        copy.wait()


def dense_operator(operator_blocks, operator_pairs, first_level, local_levels, levels):
    symmetric = 0.5 * (operator_blocks + jnp.swapaxes(operator_blocks, 1, 2))
    count = symmetric.shape[0]
    left_hot = operator_pairs[:, 0][:, None] == first_level + jnp.arange(local_levels, dtype=jnp.int32)[None]
    right_hot = operator_pairs[:, 1][:, None] == jnp.arange(levels, dtype=jnp.int32)[None]
    hot = left_hot[:, :, None, None] & right_hot[:, None, :, None]
    return jnp.sum(jnp.where(hot, symmetric.reshape(count, 1, 1, -1), 0.0), axis=0).reshape(-1)


def per_device(initial_guess, left_environment, right_environment, operator_blocks, operator_pairs):
    rows, states, window = initial_guess.shape
    levels = right_environment.shape[1]
    local_levels, n_lb = left_environment.shape[:2]
    contracted = left_environment.shape[4]
    n_rb = lax.axis_size("rb")
    line = 4 if n_rb == 16 else 2
    lines, chunk = n_rb // line, line * rows
    width, half_width = states * window, states * window // 2
    block_rows = n_lb * rows
    operator = dense_operator(
        operator_blocks, operator_pairs, lax.axis_index("wa") * local_levels, local_levels, levels
    )
    dims = (n_lb, n_rb, line, rows, states, window, levels, local_levels)
    f32, bf16 = jnp.float32, jnp.bfloat16
    dma = pltpu.SemaphoreType.DMA
    vmem = pl.BlockSpec(memory_space=pltpu.VMEM)
    out = jax.ShapeDtypeStruct((2, rows, half_width), f32)
    outs = pl.pallas_call(
        functools.partial(kernel, dims),
        out_shape=(out, out),
        in_specs=[vmem, vmem, pl.BlockSpec(memory_space=pltpu.SMEM), pl.BlockSpec(memory_space=pl.ANY)],
        out_specs=(vmem, vmem),
        scratch_shapes=[
            pltpu.VMEM((lines, block_rows, local_levels * chunk), bf16),
            pltpu.VMEM((local_levels, 2, width, half_width), bf16),
            pltpu.VMEM((window * levels, window), f32),
            pltpu.VMEM((levels, window, window), f32),
            pltpu.VMEM((STEPS, 2, contracted, half_width), bf16),
            pltpu.VMEM((STEPS, n_lb, rows, half_width), bf16),
            pltpu.VMEM((2, local_levels * chunk, half_width), bf16),
            pltpu.VMEM((2, block_rows, half_width), f32),
            pltpu.VMEM((STEPS, block_rows, half_width), bf16),
            pltpu.VMEM((STEPS, block_rows, half_width), bf16),
            pltpu.VMEM((STEPS, n_lb, rows, half_width), bf16),
            pltpu.VMEM((STEPS, n_lb, rows, half_width), bf16),
            pltpu.VMEM((2, rows, half_width), f32),
            pltpu.VMEM((rows, half_width), f32),
            pltpu.VMEM((STEPS, rows, half_width), f32),
            pltpu.VMEM((STEPS, rows, half_width), f32),
            pltpu.VMEM((STEPS, *TILE), f32),
            pltpu.VMEM((STEPS, 2 * n_lb, *TILE), f32),
            pltpu.VMEM((STEPS, *TILE), f32),
            pltpu.VMEM((STEPS, n_rb, *TILE), f32),
            dma(()),
            dma((STEPS,)),
            dma((STEPS, lines)),
            dma((STEPS, lines)),
            dma((STEPS, lines)),
            dma((STEPS,)),
            dma((STEPS,)),
            dma((STEPS,)),
            dma((STEPS,)),
            dma((STEPS,)),
            dma((STEPS,)),
            dma((STEPS,)),
            dma((STEPS,)),
            dma((STEPS,)),
            dma((STEPS,)),
            dma((2,)),
            dma((4,)),
        ],
        compiler_params=pltpu.CompilerParams(collective_id=0, has_side_effects=True),
        name="davidson",
    )(
        initial_guess.reshape(rows, width),
        right_environment,
        operator,
        left_environment.reshape(local_levels, block_rows, contracted),
    )
    return tuple(
        o.reshape(2, rows, states // 2, window).transpose(1, 0, 2, 3).reshape(rows, states, window) for o in outs
    )


def solution(mesh):
    in_specs = (P(LB_RB, None, None), P("wa", None, "rb", None, "lb"), P(), P(), P())
    out_specs = (P(LB_RB, None, None), P(LB_RB, None, None))
    return jax.shard_map(per_device, mesh=mesh, in_specs=in_specs, out_specs=out_specs, check_vma=False)
```

```python
import functools

import jax
import jax.numpy as jnp
from jax import lax
from jax.experimental import pallas as pl
from jax.experimental.pallas import tpu as pltpu
from jax.sharding import PartitionSpec as P

ITERS = 3
SWEEPS = 8
STEPS = ITERS + 1
TILE = (8, 128)
LB_RB = ("lb", "rb")
MESH_ID = pl.DeviceIdType.MESH

highest = lax.Precision.HIGHEST
epsilon = 1e-06


def rotate(matrix, vectors, p, q, order):
    y = 2.0 * matrix[p][q]
    x = matrix[q][q] - matrix[p][p]
    square = x * x + y * y
    usable = square > 0.0
    inverse = lax.rsqrt(jnp.where(usable, square, 1.0))
    half_sum = 0.5 + 0.5 * jnp.abs(x * inverse)
    inverse_large = lax.rsqrt(half_sum)
    large = half_sum * inverse_large
    small = 0.5 * jnp.abs(y * inverse) * inverse_large
    forward = x >= 0.0
    cosine = jnp.where(usable, jnp.where(forward, large, small), 1.0)
    sine = jnp.where(usable, jnp.where(forward, small, large), 0.0)
    sine = jnp.where(y < 0.0, -sine, sine)
    m_pp, m_qq, m_pq = matrix[p][p], matrix[q][q], matrix[p][q]
    cc, ss, cs = cosine * cosine, sine * sine, cosine * sine
    cross = 2.0 * cs * m_pq
    matrix[p][p] = cc * m_pp - cross + ss * m_qq
    matrix[q][q] = ss * m_pp + cross + cc * m_qq
    matrix[p][q] = matrix[q][p] = jnp.zeros_like(m_pq)
    for i in range(order):
        if i != p and i != q:
            a, b = matrix[i][p], matrix[i][q]
            matrix[i][p] = matrix[p][i] = cosine * a - sine * b
            matrix[i][q] = matrix[q][i] = sine * a + cosine * b
        a, b = vectors[i][p], vectors[i][q]
        vectors[i][p] = cosine * a - sine * b
        vectors[i][q] = sine * a + cosine * b


def lowest(entries, order):
    if order == 1:
        return entries[0][0], [jnp.ones(TILE, jnp.float32)]
    scale = jnp.abs(entries[0][0])
    for i in range(order):
        for j in range(i, order):
            scale = jnp.maximum(scale, jnp.abs(entries[i][j]))
    inverse = 1.0 / jnp.where(scale > 0.0, scale, 1.0)
    flat = [entries[i][j] * inverse for i in range(order) for j in range(order)]
    flat += [jnp.full(TILE, 1.0 if i == j else 0.0, jnp.float32) for i in range(order) for j in range(order)]

    def sweep(_, flat):
        matrix = [list(flat[i * order : (i + 1) * order]) for i in range(order)]
        base = order * order
        vectors = [list(flat[base + i * order : base + (i + 1) * order]) for i in range(order)]
        for p in range(order):
            for q in range(p + 1, order):
                rotate(matrix, vectors, p, q, order)
        return tuple(v for row in matrix + vectors for v in row)

    flat = lax.fori_loop(0, 1 if order == 2 else SWEEPS, sweep, tuple(flat))
    matrix = [flat[i * order : (i + 1) * order] for i in range(order)]
    base = order * order
    vectors = [flat[base + i * order : base + (i + 1) * order] for i in range(order)]
    best = matrix[0][0]
    weights = [vectors[i][0] for i in range(order)]
    for j in range(1, order):
        less = matrix[j][j] < best
        best = jnp.where(less, matrix[j][j], best)
        weights = [jnp.where(less, vectors[i][j], weights[i]) for i in range(order)]
    negative = weights[0] < 0.0
    weights = [jnp.where(negative, -w, w) for w in weights]
    return best * scale, weights


def kernel(
    dims,
    guess_ref,
    right_ref,
    blocks_ref,
    pairs_ref,
    left_hbm,
    vector_ref,
    residual_ref,
    left,
    mixing,
    right_rows,
    right_by_level,
    right_diag,
    gathered,
    column,
    inner,
    image,
    pair_out,
    pair_in,
    block_out,
    block_in,
    diag_parts,
    diag_in,
    basis,
    images,
    tile_out,
    tiles_a,
    tile_mid,
    tiles_b,
    final_out,
    final_in,
    left_sem,
    x_send,
    x_recv,
    f_send,
    f_recv,
    z_send,
    z_recv,
    c_send,
    c_recv,
    p_send,
    p_recv,
    s_send,
    s_recv,
    a_send,
    a_recv,
    b_send,
    b_recv,
    d_sems,
    o_sems,
):
    n_lb, n_rb, line, rows, states, window, levels, local_levels, count = dims
    lines = n_rb // line
    chunk = line * rows
    half_width = states * window // 2
    block_rows = n_lb * rows
    scale = 1.0 / (n_lb * n_rb * rows * states * window)
    z = lax.axis_index("lb")
    me = lax.axis_index("rb")
    half = lax.axis_index("wa")
    other = 1 - half
    my_line = lax.div(me, line)
    f32, bf16 = jnp.float32, jnp.bfloat16

    def remote(src, dst, send, recv, peer):
        return pltpu.make_async_remote_copy(
            src_ref=src, dst_ref=dst, send_sem=send, recv_sem=recv, device_id=peer, device_id_type=MESH_ID
        )

    def drain(region, sem):
        pltpu.make_async_copy(region, region, sem).wait()

    def each(count, body):
        def step(i, carry):
            body(i)
            return carry

        lax.fori_loop(0, count, step, 0)

    def left_copy(i):
        w, q = lax.div(i, lines), lax.rem(i, lines)
        return pltpu.make_async_copy(
            left_hbm.at[w, :, pl.ds(pl.multiple_of(q * chunk, chunk), chunk)],
            left.at[q, :, pl.ds(pl.multiple_of(w * chunk, chunk), chunk)],
            left_sem,
        )

    each(local_levels * lines, lambda i: left_copy(i).start())

    barrier = pltpu.get_barrier_semaphore()

    def greet(peer):
        pl.semaphore_signal(barrier, inc=1, device_id=peer, device_id_type=MESH_ID)

    each(n_rb - 1, lambda j: greet({"rb": lax.rem(me + 1 + j, n_rb)}))
    each(n_lb - 1, lambda j: greet({"lb": lax.rem(z + 1 + j, n_lb)}))
    each(n_lb, lambda j: greet({"lb": lax.rem(z + j, n_lb), "wa": other}))

    def own(it):
        return gathered.at[it, half, pl.ds(pl.multiple_of(me * rows, rows), rows)]

    def hand_out(it, part):
        own(it)[...] = part
        column[it, half, z] = part

    def start_hand_out(it):
        def to_plane(j):
            j = j + 1
            away, across = lax.div(j, line), lax.rem(me + j, line)
            if lines == 4:
                away = 4 * lax.div(away + 3, 4) - (away + lax.div(away, 2) - 2 * lax.div(away, 3))
            else:
                away = lines * lax.div(away + lines - 1, lines) - away
            peer = lax.rem(my_line + away, lines) * line + across
            remote(own(it), own(it), x_send.at[it], x_recv.at[it, my_line], {"rb": peer}).start()

        def to_column(j):
            remote(column.at[it, half, z], column.at[it, half, z], z_send.at[it], z_recv.at[it], {"lb": lax.rem(z + 1 + j, n_lb)}).start()

        each(n_rb - 1, to_plane)
        each(n_lb - 1, to_column)

    def own_half(ref):
        return jnp.where(half == 0, ref[:, :half_width], ref[:, half_width:])

    first = own_half(guess_ref)
    hand_out(0, first)
    current = first.astype(f32)
    pl.semaphore_wait(barrier, (n_rb - 1) + (n_lb - 1) + n_lb)
    start_hand_out(0)

    right_rows[...] = right_ref[...].astype(f32).reshape(window * levels, window)
    for v in range(levels):
        right_by_level[v] = right_rows[pl.ds(v, window, stride=levels), :]

    def factor(n, w, t, s):
        named = jnp.where(pairs_ref[0, n] == half * local_levels + w, 0.5, 0.0)
        return named * (blocks_ref[t, s, n] + blocks_ref[s, t, n])

    def mix_level(w):
        for t in range(states):
            for s in range(t, states):

                def add_block(n, tile):
                    return tile + factor(n, w, t, s) * right_by_level[pairs_ref[1, n]]

                tile = lax.fori_loop(0, count, add_block, jnp.zeros((window, window), f32), unroll=4).astype(bf16)
                for a, b in {(t, s), (s, t)}:
                    mixing[w, a // 2, b * window : (b + 1) * window, (a % 2) * window : (a % 2 + 1) * window] = tile

    each(local_levels, mix_level)

    row_at = lax.broadcasted_iota(jnp.int32, (window, window), 0)
    col_at = lax.broadcasted_iota(jnp.int32, (window, window), 1)
    for v in range(levels):
        on_diagonal = jnp.where(row_at == col_at, right_by_level[v], 0.0)
        right_diag[v] = jnp.broadcast_to(jnp.sum(on_diagonal, axis=0, keepdims=True), TILE)
    each(local_levels * lines, lambda i: left_copy(i).wait())
    q_own = my_line
    inside = lax.rem(me, line) * rows
    at_row = lax.broadcasted_iota(jnp.int32, (rows, chunk), 0)
    at_col = lax.broadcasted_iota(jnp.int32, (rows, chunk), 1)
    picked = at_col == at_row + inside
    parts = [jnp.zeros((rows, window), f32) for _ in range(states)]
    for w in range(local_levels):
        entries = left[q_own, pl.ds(pl.multiple_of(z * rows, rows), rows), w * chunk : (w + 1) * chunk].astype(f32)
        left_diag = jnp.sum(jnp.where(picked, entries, 0.0), axis=1, keepdims=True)
        for s in range(states):
            along = lax.fori_loop(
                0, count, lambda n, a, s=s, w=w: a + factor(n, w, s, s) * right_diag[pairs_ref[1, n]], jnp.zeros(TILE, f32)
            )
            parts[s] = parts[s] + left_diag * along[0:1]
    for s in range(states):
        diag_parts[s // 2, :, (s % 2) * window : (s % 2 + 1) * window] = parts[s]
    diag_copy = remote(diag_parts.at[other], diag_in, d_sems.at[0], d_sems.at[1], {"wa": other})
    diag_copy.start()

    def spread(number):
        piece = jnp.broadcast_to(number[0:1, :], (rows, TILE[1]))
        return jnp.concatenate([piece] * (half_width // TILE[1]), axis=1)

    def fold(value):
        groups = jnp.sum(value.reshape(rows // TILE[0], TILE[0], half_width), axis=0)
        out = groups[:, : TILE[1]]
        for i in range(1, half_width // TILE[1]):
            out = out + groups[:, i * TILE[1] : (i + 1) * TILE[1]]
        return out

    def chunk_rows(q):
        return pl.ds(pl.multiple_of(q * chunk, chunk), chunk)

    def line_at(i):
        if lines == 4:
            i = i + lax.div(i, 2) - 2 * lax.div(i, 3)
        return lax.rem(my_line + i, lines)

    def forward(it, q):
        region = gathered.at[it, half, chunk_rows(q)]
        return remote(region, region, f_send.at[it, q], f_recv.at[it, q], {"wa": other})

    def forward_column(it):
        region = column.at[it, half]
        return remote(region, region, c_send.at[it], c_recv.at[it], {"wa": other})

    def multiply(it, q):
        x = jnp.concatenate([gathered[it, 0, chunk_rows(q), :], gathered[it, 1, chunk_rows(q), :]], axis=1)

        for h in range(2):
            for w in range(local_levels):
                inner[h, w * chunk : (w + 1) * chunk, :] = jnp.dot(
                    x, mixing[w, h], preferred_element_type=f32
                ).astype(bf16)
        for h in range(2):
            image[h] += jnp.dot(left[q], inner[h], preferred_element_type=f32)

    def apply(it, member):
        image[...] = jnp.zeros_like(image)
        drain(gathered.at[it, half, pl.ds(0, chunk - rows)], x_recv.at[it, my_line])
        forward(it, my_line).start()

        def one_line(i):
            @pl.when(i < lines - 1)
            def _():
                q = line_at(i + 1)
                drain(gathered.at[it, half, chunk_rows(q)], x_recv.at[it, q])
                forward(it, q).start()

            @pl.when(i == lines - 1)
            def _():
                drain(column.at[it, half, pl.ds(0, n_lb - 1)], z_recv.at[it])
                forward_column(it).start()

            q = line_at(i)
            drain(gathered.at[it, other, chunk_rows(q)], f_recv.at[it, q])
            multiply(it, q)

        each(lines, one_line)

        pair_out[it] = image[other].astype(bf16)
        pair = remote(pair_out.at[it], pair_in.at[it], p_send.at[it], p_recv.at[it], {"wa": other})
        pair.start()
        sums = [fold(member * member)]
        sums += [fold(basis[j] * member) for j in range(it)]
        sums += [fold(images[j] * member) for j in range(it)]
        drain(column.at[it, other], c_recv.at[it])
        product = jnp.zeros(TILE, f32)
        for h in range(2):
            for b in range(n_lb):
                product = product + fold(image[h, b * rows : (b + 1) * rows, :] * column[it, h, b].astype(f32))
        row = lax.broadcasted_iota(jnp.int32, TILE, 0)
        tile = jnp.zeros(TILE, f32)
        for i, value in enumerate([product] + sums):
            value = jnp.sum(value, axis=0, keepdims=True)
            tile = jnp.where(row == i, jnp.broadcast_to(value, TILE), tile)

        def to_block(j):
            b = lax.rem(z + 1 + j, n_lb)
            remote(block_out.at[it, b], block_in.at[it, z], s_send.at[it], s_recv.at[it], {"lb": b}).start()

        def exchange_blocks():
            pair.wait_recv()
            summed = image[half] + pair_in[it].astype(f32)
            image[half] = summed
            block_out[it] = summed.astype(bf16).reshape(n_lb, rows, half_width)
            each(n_lb - 1, to_block)

        totals = add_up(it, tile, exchange_blocks)

        drain(block_in.at[it, pl.ds(0, n_lb - 1)], s_recv.at[it])
        total = image[half, pl.ds(pl.multiple_of(z * rows, rows), rows), :]
        for j in range(1, n_lb):
            total = total + block_in[it, lax.rem(z + j, n_lb)].astype(f32)
        return total, totals

    def add_up(it, tile, between):
        slot = z * 2 + half
        tile_out[it] = tile

        def to_column(j):
            peer = {"lb": lax.rem(z + 1 + j, n_lb), "wa": 1}
            remote(tile_out.at[it], tiles_a.at[it, slot], a_send.at[it], a_recv.at[it], peer).start()

        each(n_lb - 1, to_column)

        @pl.when(half == 0)
        def _():
            remote(tile_out.at[it], tiles_a.at[it, slot], a_send.at[it], a_recv.at[it], {"wa": 1}).start()

        @pl.when(half == 1)
        def _():
            tiles_a[it, slot] = tile

        between()

        @pl.when(half == 1)
        def _():
            drain(tiles_a.at[it, pl.ds(0, 2 * n_lb - 1)], a_recv.at[it])
            summed = tiles_a[it, 0]
            for j in range(1, 2 * n_lb):
                summed = summed + tiles_a[it, j]
            tile_mid[it] = summed
            tiles_b[it, me] = summed

            def to_plane(j):
                peer = {"rb": lax.rem(me + lax.div(j + 1, 2), n_rb), "wa": lax.rem(j, 2)}
                remote(tile_mid.at[it], tiles_b.at[it, me], b_send.at[it], b_recv.at[it], peer).start()

            each(2 * n_rb - 1, to_plane)
            drain(tiles_b.at[it, pl.ds(0, n_rb - 1)], b_recv.at[it])

        @pl.when(half == 0)
        def _():
            drain(tiles_b.at[it], b_recv.at[it])

        tile = tiles_b[it, 0]
        for j in range(1, n_rb):
            tile = tile + tiles_b[it, j]
        tile = jnp.broadcast_to(jnp.sum(tile, axis=1, keepdims=True), TILE) * scale
        return [jnp.broadcast_to(tile[i : i + 1, :], TILE) for i in range(2 + 2 * it)]

    entries = [[None] * STEPS for _ in range(STEPS)]
    diagonal = None
    for it in range(STEPS):
        applied, totals = apply(it, current)
        energy, square = totals[0], totals[1]
        overlaps, crossed = totals[2 : 2 + it], totals[2 + it :]
        norm = square
        for a in overlaps:
            norm = norm - a * a
        inverse = lax.rsqrt(jnp.maximum(norm, 0.0) + epsilon)
        for j in range(it):
            value = crossed[j]
            for i in range(it):
                value = value - overlaps[i] * entries[i][j]
            entries[j][it] = entries[it][j] = inverse * value
            energy = energy - overlaps[j] * (crossed[j] + value)
        entries[it][it] = inverse * inverse * energy
        theta, weights = lowest(entries, it + 1)

        vector, applied_now = current, applied
        for j in range(it):
            a = spread(overlaps[j])
            vector = vector - a * basis[j]
            applied_now = applied_now - a * images[j]
        grow = spread(inverse)
        vector, applied_now = vector * grow, applied_now * grow
        basis[it] = vector
        images[it] = applied_now
        last = spread(weights[it])
        ritz, residual = last * vector, last * applied_now
        for j in range(it):
            a = spread(weights[j])
            ritz = ritz + a * basis[j]
            residual = residual + a * images[j]
        shift = spread(theta)
        residual = residual - shift * ritz
        if it == 0:
            diag_copy.wait()
            diagonal = diag_parts[half] + diag_in[...]
            diag_parts[half] = diagonal
        if it < ITERS:
            current = residual / (jnp.abs(diag_parts[half] - shift) + 1.0)
            hand_out(it + 1, current.astype(bf16))
            start_hand_out(it + 1)

    outputs = (vector_ref, residual_ref)
    for i, value in enumerate((ritz, residual)):
        final_out[i] = value
    last_copy = remote(final_out, final_in, o_sems.at[0], o_sems.at[1], {"wa": other})
    last_copy.start()

    def put(i, side, value):
        for k in range(states // 2):
            outputs[i][pl.ds(side * (states // 2) + k, rows, stride=states), :] = value[:, k * window : (k + 1) * window]

    for side in range(2):

        @pl.when(half == side)
        def _():
            for i, value in enumerate((ritz, residual)):
                put(i, side, value)

    def finish(it):
        drain(gathered.at[it, 0, pl.ds(0, (n_rb - 1) * rows)], x_send.at[it])
        drain(column.at[it, half, pl.ds(0, n_lb - 1)], z_send.at[it])
        forward_column(it).wait_send()
        each(lines, lambda q: forward(it, q).wait_send())
        drain(pair_out.at[it], p_send.at[it])
        drain(block_out.at[it, pl.ds(0, n_lb - 1)], s_send.at[it])
        drain(tiles_a.at[it, pl.ds(0, n_lb - 1)], a_send.at[it])

        @pl.when(half == 0)
        def _():
            drain(tiles_a.at[it, 0], a_send.at[it])

        @pl.when(half == 1)
        def _():
            drain(tiles_b.at[it], b_send.at[it])
            drain(tiles_b.at[it, pl.ds(0, n_rb - 1)], b_send.at[it])

    each(STEPS, finish)
    last_copy.wait()
    for side in range(2):

        @pl.when(half == 1 - side)
        def _():
            for i in range(2):
                put(i, side, final_in[i])


def per_device(initial_guess, left_environment, right_environment, operator_blocks, operator_pairs):
    rows, states, window = initial_guess.shape
    levels = right_environment.shape[1]
    local_levels, n_lb = left_environment.shape[:2]
    contracted = left_environment.shape[4]
    n_rb = lax.axis_size("rb")
    line = 4 if n_rb == 16 else 2
    lines, chunk = n_rb // line, line * rows
    width, half_width = states * window, states * window // 2
    block_rows = n_lb * rows
    dims = (n_lb, n_rb, line, rows, states, window, levels, local_levels, operator_pairs.shape[0])
    f32, bf16 = jnp.float32, jnp.bfloat16
    dma = pltpu.SemaphoreType.DMA
    vmem = pl.BlockSpec(memory_space=pltpu.VMEM)
    smem = pl.BlockSpec(memory_space=pltpu.SMEM)
    out = jax.ShapeDtypeStruct((rows * states, window), f32)
    outs = pl.pallas_call(
        functools.partial(kernel, dims),
        out_shape=(out, out),
        in_specs=[vmem, vmem, smem, smem, pl.BlockSpec(memory_space=pl.ANY)],
        out_specs=(vmem, vmem),
        scratch_shapes=[
            pltpu.VMEM((lines, block_rows, local_levels * chunk), bf16),
            pltpu.VMEM((local_levels, 2, width, half_width), bf16),
            pltpu.VMEM((window * levels, window), f32),
            pltpu.VMEM((levels, window, window), f32),
            pltpu.VMEM((levels, *TILE), f32),
            pltpu.VMEM((STEPS, 2, contracted, half_width), bf16),
            pltpu.VMEM((STEPS, 2, n_lb, rows, half_width), bf16),
            pltpu.VMEM((2, local_levels * chunk, half_width), bf16),
            pltpu.VMEM((2, block_rows, half_width), f32),
            pltpu.VMEM((STEPS, block_rows, half_width), bf16),
            pltpu.VMEM((STEPS, block_rows, half_width), bf16),
            pltpu.VMEM((STEPS, n_lb, rows, half_width), bf16),
            pltpu.VMEM((STEPS, n_lb, rows, half_width), bf16),
            pltpu.VMEM((2, rows, half_width), f32),
            pltpu.VMEM((rows, half_width), f32),
            pltpu.VMEM((STEPS, rows, half_width), f32),
            pltpu.VMEM((STEPS, rows, half_width), f32),
            pltpu.VMEM((STEPS, *TILE), f32),
            pltpu.VMEM((STEPS, 2 * n_lb, *TILE), f32),
            pltpu.VMEM((STEPS, *TILE), f32),
            pltpu.VMEM((STEPS, n_rb, *TILE), f32),
            pltpu.VMEM((2, rows, half_width), f32),
            pltpu.VMEM((2, rows, half_width), f32),
            dma(()),
            dma((STEPS,)),
            dma((STEPS, lines)),
            dma((STEPS, lines)),
            dma((STEPS, lines)),
            dma((STEPS,)),
            dma((STEPS,)),
            dma((STEPS,)),
            dma((STEPS,)),
            dma((STEPS,)),
            dma((STEPS,)),
            dma((STEPS,)),
            dma((STEPS,)),
            dma((STEPS,)),
            dma((STEPS,)),
            dma((STEPS,)),
            dma((STEPS,)),
            dma((2,)),
            dma((2,)),
        ],
        compiler_params=pltpu.CompilerParams(collective_id=0, has_side_effects=True),
        name="davidson",
    )(
        initial_guess.reshape(rows, width),
        right_environment,
        operator_blocks.transpose(1, 2, 0),
        operator_pairs.T,
        left_environment.reshape(local_levels, block_rows, contracted),
    )
    return tuple(o.reshape(rows, states, window) for o in outs)


def solution(mesh):
    in_specs = (P(LB_RB, None, None), P("wa", None, "rb", None, "lb"), P(), P(), P())
    out_specs = (P(LB_RB, None, None), P(LB_RB, None, None))
    return jax.shard_map(per_device, mesh=mesh, in_specs=in_specs, out_specs=out_specs, check_vma=False)
```

```python
import functools

import jax
import jax.numpy as jnp
from jax import lax
from jax.experimental import pallas as pl
from jax.experimental.pallas import tpu as pltpu
from jax.sharding import PartitionSpec as P

ITERS = 3
SWEEPS = 8
STEPS = ITERS + 1
TILE = (8, 128)
LB_RB = ("lb", "rb")
MESH_ID = pl.DeviceIdType.MESH

highest = lax.Precision.HIGHEST
epsilon = 1e-06


def rotate(matrix, vectors, p, q, order):
    y = 2.0 * matrix[p][q]
    x = matrix[q][q] - matrix[p][p]
    square = x * x + y * y
    usable = square > 0.0
    inverse = lax.rsqrt(jnp.where(usable, square, 1.0))
    half_sum = 0.5 + 0.5 * jnp.abs(x * inverse)
    inverse_large = lax.rsqrt(half_sum)
    large = half_sum * inverse_large
    small = 0.5 * jnp.abs(y * inverse) * inverse_large
    forward = x >= 0.0
    cosine = jnp.where(usable, jnp.where(forward, large, small), 1.0)
    sine = jnp.where(usable, jnp.where(forward, small, large), 0.0)
    sine = jnp.where(y < 0.0, -sine, sine)
    m_pp, m_qq, m_pq = matrix[p][p], matrix[q][q], matrix[p][q]
    cc, ss, cs = cosine * cosine, sine * sine, cosine * sine
    cross = 2.0 * cs * m_pq
    matrix[p][p] = cc * m_pp - cross + ss * m_qq
    matrix[q][q] = ss * m_pp + cross + cc * m_qq
    matrix[p][q] = matrix[q][p] = jnp.zeros_like(m_pq)
    for i in range(order):
        if i != p and i != q:
            a, b = matrix[i][p], matrix[i][q]
            matrix[i][p] = matrix[p][i] = cosine * a - sine * b
            matrix[i][q] = matrix[q][i] = sine * a + cosine * b
        a, b = vectors[i][p], vectors[i][q]
        vectors[i][p] = cosine * a - sine * b
        vectors[i][q] = sine * a + cosine * b


def lowest(entries, order):
    if order == 1:
        return entries[0][0], [jnp.ones(TILE, jnp.float32)]
    scale = jnp.abs(entries[0][0])
    for i in range(order):
        for j in range(i, order):
            scale = jnp.maximum(scale, jnp.abs(entries[i][j]))
    inverse = 1.0 / jnp.where(scale > 0.0, scale, 1.0)
    flat = [entries[i][j] * inverse for i in range(order) for j in range(order)]
    flat += [jnp.full(TILE, 1.0 if i == j else 0.0, jnp.float32) for i in range(order) for j in range(order)]

    def sweep(_, flat):
        matrix = [list(flat[i * order : (i + 1) * order]) for i in range(order)]
        base = order * order
        vectors = [list(flat[base + i * order : base + (i + 1) * order]) for i in range(order)]
        for p in range(order):
            for q in range(p + 1, order):
                rotate(matrix, vectors, p, q, order)
        return tuple(v for row in matrix + vectors for v in row)

    flat = lax.fori_loop(0, 1 if order == 2 else SWEEPS, sweep, tuple(flat))
    matrix = [flat[i * order : (i + 1) * order] for i in range(order)]
    base = order * order
    vectors = [flat[base + i * order : base + (i + 1) * order] for i in range(order)]
    best = matrix[0][0]
    weights = [vectors[i][0] for i in range(order)]
    for j in range(1, order):
        less = matrix[j][j] < best
        best = jnp.where(less, matrix[j][j], best)
        weights = [jnp.where(less, vectors[i][j], weights[i]) for i in range(order)]
    negative = weights[0] < 0.0
    weights = [jnp.where(negative, -w, w) for w in weights]
    return best * scale, weights


def kernel(
    dims,
    guess_ref,
    right_ref,
    blocks_ref,
    pairs_ref,
    left_hbm,
    vector_ref,
    residual_ref,
    left,
    mixing,
    right_rows,
    right_by_level,
    right_diag,
    gathered,
    column,
    inner,
    image,
    pair_out,
    pair_in,
    block_out,
    block_in,
    diag_parts,
    diag_in,
    basis,
    images,
    tile_out,
    tiles_a,
    tile_mid,
    tiles_b,
    final_out,
    final_in,
    guess_rows,
    left_sem,
    x_send,
    x_recv,
    f_send,
    f_recv,
    z_send,
    z_recv,
    c_send,
    c_recv,
    p_send,
    p_recv,
    s_send,
    s_recv,
    a_send,
    a_recv,
    b_send,
    b_recv,
    d_sems,
    o_sems,
):
    n_lb, n_rb, line, rows, states, window, levels, local_levels, count = dims
    lines = n_rb // line
    chunk = line * rows
    half_width = states * window // 2
    block_rows = n_lb * rows
    scale = 1.0 / (n_lb * n_rb * rows * states * window)
    z = lax.axis_index("lb")
    me = lax.axis_index("rb")
    half = lax.axis_index("wa")
    other = 1 - half
    my_line, my_place = lax.div(me, line), lax.rem(me, line)
    f32, bf16 = jnp.float32, jnp.bfloat16

    def remote(src, dst, send, recv, peer):
        return pltpu.make_async_remote_copy(
            src_ref=src, dst_ref=dst, send_sem=send, recv_sem=recv, device_id=peer, device_id_type=MESH_ID
        )

    def drain(region, sem):
        pltpu.make_async_copy(region, region, sem).wait()

    def each(count, body, unroll=False):
        def step(i, carry):
            body(i)
            return carry

        lax.fori_loop(0, count, step, 0, unroll=unroll)

    def left_copy(i):
        w, q = lax.div(i, lines), lax.rem(i, lines)
        return pltpu.make_async_copy(
            left_hbm.at[w, :, pl.ds(pl.multiple_of(q * chunk, chunk), chunk)],
            left.at[q, :, pl.ds(pl.multiple_of(w * chunk, chunk), chunk)],
            left_sem,
        )

    each(local_levels * lines, lambda i: left_copy(i).start())

    barrier = pltpu.get_barrier_semaphore()

    def greet(peer):
        pl.semaphore_signal(barrier, inc=1, device_id=peer, device_id_type=MESH_ID)

    each(n_rb - 1, lambda j: greet({"rb": lax.rem(me + 1 + j, n_rb)}))
    each(n_lb - 1, lambda j: greet({"lb": lax.rem(z + 1 + j, n_lb)}))
    each(n_lb, lambda j: greet({"lb": lax.rem(z + j, n_lb), "wa": other}))

    def block(it, side, x, y):
        return gathered.at[it, side, pl.ds(pl.multiple_of((x * line + y) * rows, rows), rows)]

    def send_block(it, x, y, to_x, to_y):
        region = block(it, half, x, y)
        peer = {"rb": lax.rem(to_x, lines) * line + lax.rem(to_y, line)}
        remote(region, region, x_send.at[it], x_recv.at[it, x * line + y], peer).start()

    def forward(it, x, y):
        region = block(it, half, x, y)
        remote(region, region, f_send.at[it], f_recv.at[it, x * line + y], {"wa": other}).start()

    def hand_out(it, part):
        block(it, half, my_line, my_place)[...] = part
        column[it, half, z] = part

    def far_first(j, size):
        step = lax.div(j + 1, 2)
        return size // 2 + step - 2 * step * lax.rem(j, 2)

    def start_hand_out(it):
        def to_axes(j):
            d = far_first(j, line)
            send_block(it, my_line, my_place, my_line, my_place + d)
            send_block(it, my_line, my_place, my_line + d, my_place)

        def to_column(j):
            region = column.at[it, half, z]
            remote(region, region, z_send.at[it], z_recv.at[it], {"lb": lax.rem(z + 1 + j, n_lb)}).start()

        each(line - 1, to_axes, True)
        forward(it, my_line, my_place)
        each(n_lb - 1, to_column)

    def pass_on(it):
        def one(j):
            d = j + 1 + j - 3 * lax.div(j, 2)
            on_x = 1 - lax.rem(my_line + my_place + d, 2)
            x, y = lax.rem(my_line + d * on_x, lines), lax.rem(my_place + d * (1 - on_x), line)
            drain(block(it, half, x, y), x_recv.at[it, x * line + y])

            def to(k):
                e = far_first(k, line)
                send_block(it, x, y, my_line + e * (1 - on_x), my_place + e * on_x)

            each(line - 1, to, True)
            forward(it, x, y)

        each(line - 1, one)

    def arrive(it, x):
        for y in range(line):
            same_x, same_y = x == my_line, my_place == y
            odd = lax.rem(x + y, 2) == 1
            done = (same_x & same_y) | (same_y & ~same_x & ~odd) | (same_x & ~same_y & odd)

            @pl.when(jnp.logical_not(done))
            def _():
                drain(block(it, half, x, y), x_recv.at[it, x * line + y])
                forward(it, x, y)

    for r in range(rows):
        guess_rows[r * states : (r + 1) * states, :] = guess_ref[r].astype(f32)
    first = jnp.concatenate(
        [
            guess_rows[pl.ds(half * (states // 2) + k, rows, stride=states), :].astype(bf16)
            for k in range(states // 2)
        ],
        axis=1,
    )
    hand_out(0, first)
    current = first.astype(f32)
    pl.semaphore_wait(barrier, (n_rb - 1) + (n_lb - 1) + n_lb)
    start_hand_out(0)

    right_rows[...] = right_ref[...].astype(f32).reshape(window * levels, window)
    for v in range(levels):
        right_by_level[v] = right_rows[pl.ds(v, window, stride=levels), :]

    def factor(n, w, t, s):
        named = jnp.where(pairs_ref[0, n] == half * local_levels + w, 0.5, 0.0)
        return named * (blocks_ref[t, s, n] + blocks_ref[s, t, n])

    def mix_level(w):
        for t in range(states):
            for s in range(t, states):

                def add_block(n, tile):
                    return tile + factor(n, w, t, s) * right_by_level[pairs_ref[1, n]]

                tile = lax.fori_loop(0, count, add_block, jnp.zeros((window, window), f32), unroll=4).astype(bf16)
                for a, b in {(t, s), (s, t)}:
                    mixing[w, a // 2, b * window : (b + 1) * window, (a % 2) * window : (a % 2 + 1) * window] = tile

    each(local_levels, mix_level)

    row_at = lax.broadcasted_iota(jnp.int32, (window, window), 0)
    col_at = lax.broadcasted_iota(jnp.int32, (window, window), 1)
    for v in range(levels):
        on_diagonal = jnp.where(row_at == col_at, right_by_level[v], 0.0)
        right_diag[v] = jnp.broadcast_to(jnp.sum(on_diagonal, axis=0, keepdims=True), TILE)
    each(local_levels * lines, lambda i: left_copy(i).wait())
    q_own = my_line
    inside = lax.rem(me, line) * rows
    at_row = lax.broadcasted_iota(jnp.int32, (rows, chunk), 0)
    at_col = lax.broadcasted_iota(jnp.int32, (rows, chunk), 1)
    picked = at_col == at_row + inside
    parts = [jnp.zeros((rows, window), f32) for _ in range(states)]
    for w in range(local_levels):
        entries = left[q_own, pl.ds(pl.multiple_of(z * rows, rows), rows), w * chunk : (w + 1) * chunk].astype(f32)
        left_diag = jnp.sum(jnp.where(picked, entries, 0.0), axis=1, keepdims=True)
        for s in range(states):
            along = lax.fori_loop(
                0, count, lambda n, a, s=s, w=w: a + factor(n, w, s, s) * right_diag[pairs_ref[1, n]], jnp.zeros(TILE, f32)
            )
            parts[s] = parts[s] + left_diag * along[0:1]
    for s in range(states):
        diag_parts[s // 2, :, (s % 2) * window : (s % 2 + 1) * window] = parts[s]
    diag_copy = remote(diag_parts.at[other], diag_in, d_sems.at[0], d_sems.at[1], {"wa": other})
    diag_copy.start()

    def spread(number):
        piece = jnp.concatenate([number] * (rows // TILE[0]), axis=0)
        return jnp.concatenate([piece] * (half_width // TILE[1]), axis=1)

    def fold(value):
        groups = jnp.sum(value.reshape(rows // TILE[0], TILE[0], half_width), axis=0)
        out = groups[:, : TILE[1]]
        for i in range(1, half_width // TILE[1]):
            out = out + groups[:, i * TILE[1] : (i + 1) * TILE[1]]
        return out

    def chunk_rows(q):
        return pl.ds(pl.multiple_of(q * chunk, chunk), chunk)

    def line_at(i):
        if lines == 4:
            i = i + lax.div(i, 2) - 2 * lax.div(i, 3)
        return lax.rem(my_line + i, lines)

    def forward_column(it):
        region = column.at[it, half]
        return remote(region, region, c_send.at[it], c_recv.at[it], {"wa": other})

    def multiply(it, q):
        x = jnp.concatenate([gathered[it, 0, chunk_rows(q), :], gathered[it, 1, chunk_rows(q), :]], axis=1)

        for h in range(2):
            for w in range(local_levels):
                inner[h, w * chunk : (w + 1) * chunk, :] = jnp.dot(
                    x, mixing[w, h], preferred_element_type=f32
                ).astype(bf16)
        for h in range(2):
            image[h] += jnp.dot(left[q], inner[h], preferred_element_type=f32)

    def row_sums(first_row, values):
        row = lax.broadcasted_iota(jnp.int32, TILE, 0)
        tile = jnp.zeros(TILE, f32)
        for i, value in enumerate(values):
            value = jnp.sum(value, axis=0, keepdims=True)
            tile = jnp.where(row == first_row + i, jnp.broadcast_to(value, TILE), tile)
        return tile

    def apply(it, member):
        pass_on(it)
        image[...] = jnp.zeros_like(image)
        sums = [fold(member * member)]
        sums += [fold(basis[j] * member) for j in range(it)]
        sums += [fold(images[j] * member) for j in range(it)]
        tile_out[it] = row_sums(1, sums)
        arrive(it, my_line)
        pair = remote(pair_out.at[it], pair_in.at[it], p_send.at[it], p_recv.at[it], {"wa": other})

        def one_line(i):
            @pl.when(i == lines - 1)
            def _():
                drain(column.at[it, half, pl.ds(0, n_lb - 1)], z_recv.at[it])
                forward_column(it).start()

            q = line_at(i)
            for y in range(line):
                drain(block(it, other, q, y), f_recv.at[it, q * line + y])
            multiply(it, q)

            @pl.when(i == 0)
            def _():
                arrive(it, line_at(1))

            @pl.when(i < lines - 2)
            def _():
                arrive(it, line_at(i + 2))

        each(lines, one_line)
        pair_out[it] = image[other].astype(bf16)
        pair.start()
        drain(column.at[it, other], c_recv.at[it])
        product = jnp.zeros(TILE, f32)
        for h in range(2):
            for b in range(n_lb):
                product = product + fold(image[h, b * rows : (b + 1) * rows, :] * column[it, h, b].astype(f32))
        tile = tile_out[it] + row_sums(0, [product])

        def to_block(j):
            b = lax.rem(z + far_first(j, n_lb), n_lb)
            remote(block_out.at[it, b], block_in.at[it, z], s_send.at[it], s_recv.at[it], {"lb": b}).start()

        def exchange_blocks():
            pair.wait_recv()
            summed = image[half] + pair_in[it].astype(f32)
            image[half] = summed
            block_out[it] = summed.astype(bf16).reshape(n_lb, rows, half_width)
            each(n_lb - 1, to_block, True)

        def collect():
            drain(block_in.at[it, pl.ds(0, n_lb - 1)], s_recv.at[it])
            total = image[half, pl.ds(pl.multiple_of(z * rows, rows), rows), :]
            for j in range(1, n_lb):
                total = total + block_in[it, lax.rem(z + j, n_lb)].astype(f32)
            return total

        return add_up(it, tile, exchange_blocks), collect

    def add_up(it, tile, between):
        slot = z * 2 + half
        tile_out[it] = tile

        def to_column(j):
            peer = {"lb": lax.rem(z + 1 + j, n_lb), "wa": 1}
            remote(tile_out.at[it], tiles_a.at[it, slot], a_send.at[it], a_recv.at[it], peer).start()

        each(n_lb - 1, to_column, True)

        @pl.when(half == 0)
        def _():
            remote(tile_out.at[it], tiles_a.at[it, slot], a_send.at[it], a_recv.at[it], {"wa": 1}).start()

        @pl.when(half == 1)
        def _():
            tiles_a[it, slot] = tile

        between()

        @pl.when(half == 1)
        def _():
            drain(tiles_a.at[it, pl.ds(0, 2 * n_lb - 1)], a_recv.at[it])
            summed = tiles_a[it, 0]
            for j in range(1, 2 * n_lb):
                summed = summed + tiles_a[it, j]
            tile_mid[it] = summed
            tiles_b[it, me] = summed

            def to_plane(j):
                peer = {"rb": lax.rem(me + lax.div(j + 1, 2), n_rb), "wa": lax.rem(j, 2)}
                remote(tile_mid.at[it], tiles_b.at[it, me], b_send.at[it], b_recv.at[it], peer).start()

            each(2 * n_rb - 1, to_plane, True)
            drain(tiles_b.at[it, pl.ds(0, n_rb - 1)], b_recv.at[it])

        @pl.when(half == 0)
        def _():
            drain(tiles_b.at[it], b_recv.at[it])

        tile = tiles_b[it, 0]
        for j in range(1, n_rb):
            tile = tile + tiles_b[it, j]
        tile = jnp.broadcast_to(jnp.sum(tile, axis=1, keepdims=True), TILE) * scale
        return [jnp.broadcast_to(tile[i : i + 1, :], TILE) for i in range(2 + 2 * it)]

    entries = [[None] * STEPS for _ in range(STEPS)]
    diagonal = None
    for it in range(STEPS):
        totals, collect = apply(it, current)
        energy, square = totals[0], totals[1]
        overlaps, crossed = totals[2 : 2 + it], totals[2 + it :]
        norm = square
        for a in overlaps:
            norm = norm - a * a
        inverse = lax.rsqrt(jnp.maximum(norm, 0.0) + epsilon)
        for j in range(it):
            value = crossed[j]
            for i in range(it):
                value = value - overlaps[i] * entries[i][j]
            entries[j][it] = entries[it][j] = inverse * value
            energy = energy - overlaps[j] * (crossed[j] + value)
        entries[it][it] = inverse * inverse * energy
        theta, weights = lowest(entries, it + 1)

        vector, applied_now = current, collect()
        for j in range(it):
            a = spread(overlaps[j])
            vector = vector - a * basis[j]
            applied_now = applied_now - a * images[j]
        grow = spread(inverse)
        vector, applied_now = vector * grow, applied_now * grow
        basis[it] = vector
        images[it] = applied_now
        last = spread(weights[it])
        ritz, residual = last * vector, last * applied_now
        for j in range(it):
            a = spread(weights[j])
            ritz = ritz + a * basis[j]
            residual = residual + a * images[j]
        shift = spread(theta)
        residual = residual - shift * ritz
        if it == 0:
            diag_copy.wait()
            diagonal = diag_parts[half] + diag_in[...]
            diag_parts[half] = diagonal
        if it < ITERS:
            current = residual / (jnp.abs(diag_parts[half] - shift) + 1.0)
            hand_out(it + 1, current.astype(bf16))
            start_hand_out(it + 1)

    outputs = (vector_ref, residual_ref)
    for i, value in enumerate((ritz, residual)):
        final_out[i] = value
    last_copy = remote(final_out, final_in, o_sems.at[0], o_sems.at[1], {"wa": other})
    last_copy.start()

    def put(i, side, value):
        for k in range(states // 2):
            outputs[i][pl.ds(side * (states // 2) + k, rows, stride=states), :] = value[:, k * window : (k + 1) * window]

    for side in range(2):

        @pl.when(half == side)
        def _():
            for i, value in enumerate((ritz, residual)):
                put(i, side, value)

    def finish(it):
        drain(gathered.at[it, 0, pl.ds(0, (n_rb - 1) * rows)], x_send.at[it])
        drain(column.at[it, half, pl.ds(0, n_lb - 1)], z_send.at[it])
        forward_column(it).wait_send()
        drain(gathered.at[it, half], f_send.at[it])
        drain(pair_out.at[it], p_send.at[it])
        drain(block_out.at[it, pl.ds(0, n_lb - 1)], s_send.at[it])
        drain(tiles_a.at[it, pl.ds(0, n_lb - 1)], a_send.at[it])

        @pl.when(half == 0)
        def _():
            drain(tiles_a.at[it, 0], a_send.at[it])

        @pl.when(half == 1)
        def _():
            drain(tiles_b.at[it], b_send.at[it])
            drain(tiles_b.at[it, pl.ds(0, n_rb - 1)], b_send.at[it])

    each(STEPS, finish)
    last_copy.wait()
    for side in range(2):

        @pl.when(half == 1 - side)
        def _():
            for i in range(2):
                put(i, side, final_in[i])


def per_device(initial_guess, left_environment, right_environment, operator_blocks, operator_pairs):
    rows, states, window = initial_guess.shape
    levels = right_environment.shape[1]
    local_levels, n_lb = left_environment.shape[:2]
    contracted = left_environment.shape[4]
    n_rb = lax.axis_size("rb")
    line = 4 if n_rb == 16 else 2
    lines, chunk = n_rb // line, line * rows
    width, half_width = states * window, states * window // 2
    block_rows = n_lb * rows
    dims = (n_lb, n_rb, line, rows, states, window, levels, local_levels, operator_pairs.shape[0])
    f32, bf16 = jnp.float32, jnp.bfloat16
    dma = pltpu.SemaphoreType.DMA
    vmem = pl.BlockSpec(memory_space=pltpu.VMEM)
    smem = pl.BlockSpec(memory_space=pltpu.SMEM)
    out = jax.ShapeDtypeStruct((rows * states, window), f32)
    outs = pl.pallas_call(
        functools.partial(kernel, dims),
        out_shape=(out, out),
        in_specs=[vmem, vmem, smem, smem, pl.BlockSpec(memory_space=pltpu.HBM)],
        out_specs=(vmem, vmem),
        scratch_shapes=[
            pltpu.VMEM((lines, block_rows, local_levels * chunk), bf16),
            pltpu.VMEM((local_levels, 2, width, half_width), bf16),
            pltpu.VMEM((window * levels, window), f32),
            pltpu.VMEM((levels, window, window), f32),
            pltpu.VMEM((levels, *TILE), f32),
            pltpu.VMEM((STEPS, 2, contracted, half_width), bf16),
            pltpu.VMEM((STEPS, 2, n_lb, rows, half_width), bf16),
            pltpu.VMEM((2, local_levels * chunk, half_width), bf16),
            pltpu.VMEM((2, block_rows, half_width), f32),
            pltpu.VMEM((STEPS, block_rows, half_width), bf16),
            pltpu.VMEM((STEPS, block_rows, half_width), bf16),
            pltpu.VMEM((STEPS, n_lb, rows, half_width), bf16),
            pltpu.VMEM((STEPS, n_lb, rows, half_width), bf16),
            pltpu.VMEM((2, rows, half_width), f32),
            pltpu.VMEM((rows, half_width), f32),
            pltpu.VMEM((STEPS, rows, half_width), f32),
            pltpu.VMEM((STEPS, rows, half_width), f32),
            pltpu.VMEM((STEPS, *TILE), f32),
            pltpu.VMEM((STEPS, 2 * n_lb, *TILE), f32),
            pltpu.VMEM((STEPS, *TILE), f32),
            pltpu.VMEM((STEPS, n_rb, *TILE), f32),
            pltpu.VMEM((2, rows, half_width), f32),
            pltpu.VMEM((2, rows, half_width), f32),
            pltpu.VMEM((rows * states, window), f32),
            dma(()),
            dma((STEPS,)),
            dma((STEPS, n_rb)),
            dma((STEPS,)),
            dma((STEPS, n_rb)),
            dma((STEPS,)),
            dma((STEPS,)),
            dma((STEPS,)),
            dma((STEPS,)),
            dma((STEPS,)),
            dma((STEPS,)),
            dma((STEPS,)),
            dma((STEPS,)),
            dma((STEPS,)),
            dma((STEPS,)),
            dma((STEPS,)),
            dma((STEPS,)),
            dma((2,)),
            dma((2,)),
        ],
        compiler_params=pltpu.CompilerParams(collective_id=0, has_side_effects=True),
        name="davidson",
    )(
        initial_guess,
        right_environment,
        operator_blocks.transpose(1, 2, 0),
        operator_pairs.T,
        left_environment.reshape(local_levels, block_rows, contracted),
    )
    return tuple(o.reshape(rows, states, window) for o in outs)


def solution(mesh):
    in_specs = (P(LB_RB, None, None), P("wa", None, "rb", None, "lb"), P(), P(), P())
    out_specs = (P(LB_RB, None, None), P(LB_RB, None, None))
    return jax.shard_map(per_device, mesh=mesh, in_specs=in_specs, out_specs=out_specs, check_vma=False)
```

```python
import functools

import jax
import jax.numpy as jnp
from jax import lax
from jax.experimental import pallas as pl
from jax.experimental.pallas import tpu as pltpu
from jax.sharding import PartitionSpec as P

ITERS = 3
SWEEPS = 8
STEPS = ITERS + 1
TILE = (8, 128)
LB_RB = ("lb", "rb")
MESH_ID = pl.DeviceIdType.MESH

highest = lax.Precision.HIGHEST
epsilon = 1e-06


def rotate(matrix, vectors, p, q, order):
    y = 2.0 * matrix[p][q]
    x = matrix[q][q] - matrix[p][p]
    square = x * x + y * y
    usable = square > 0.0
    inverse = lax.rsqrt(jnp.where(usable, square, 1.0))
    half_sum = 0.5 + 0.5 * jnp.abs(x * inverse)
    inverse_large = lax.rsqrt(half_sum)
    large = half_sum * inverse_large
    small = 0.5 * jnp.abs(y * inverse) * inverse_large
    forward = x >= 0.0
    cosine = jnp.where(usable, jnp.where(forward, large, small), 1.0)
    sine = jnp.where(usable, jnp.where(forward, small, large), 0.0)
    sine = jnp.where(y < 0.0, -sine, sine)
    m_pp, m_qq, m_pq = matrix[p][p], matrix[q][q], matrix[p][q]
    cc, ss, cs = cosine * cosine, sine * sine, cosine * sine
    cross = 2.0 * cs * m_pq
    matrix[p][p] = cc * m_pp - cross + ss * m_qq
    matrix[q][q] = ss * m_pp + cross + cc * m_qq
    matrix[p][q] = matrix[q][p] = jnp.zeros_like(m_pq)
    for i in range(order):
        if i != p and i != q:
            a, b = matrix[i][p], matrix[i][q]
            matrix[i][p] = matrix[p][i] = cosine * a - sine * b
            matrix[i][q] = matrix[q][i] = sine * a + cosine * b
        a, b = vectors[i][p], vectors[i][q]
        vectors[i][p] = cosine * a - sine * b
        vectors[i][q] = sine * a + cosine * b


def lowest(entries, order):
    if order == 1:
        return entries[0][0], [jnp.ones(TILE, jnp.float32)]
    scale = jnp.abs(entries[0][0])
    for i in range(order):
        for j in range(i, order):
            scale = jnp.maximum(scale, jnp.abs(entries[i][j]))
    inverse = 1.0 / jnp.where(scale > 0.0, scale, 1.0)
    flat = [entries[i][j] * inverse for i in range(order) for j in range(order)]
    flat += [jnp.full(TILE, 1.0 if i == j else 0.0, jnp.float32) for i in range(order) for j in range(order)]

    def sweep(_, flat):
        matrix = [list(flat[i * order : (i + 1) * order]) for i in range(order)]
        base = order * order
        vectors = [list(flat[base + i * order : base + (i + 1) * order]) for i in range(order)]
        for p in range(order):
            for q in range(p + 1, order):
                rotate(matrix, vectors, p, q, order)
        return tuple(v for row in matrix + vectors for v in row)

    flat = lax.fori_loop(0, 1 if order == 2 else SWEEPS, sweep, tuple(flat))
    matrix = [flat[i * order : (i + 1) * order] for i in range(order)]
    base = order * order
    vectors = [flat[base + i * order : base + (i + 1) * order] for i in range(order)]
    best = matrix[0][0]
    weights = [vectors[i][0] for i in range(order)]
    for j in range(1, order):
        less = matrix[j][j] < best
        best = jnp.where(less, matrix[j][j], best)
        weights = [jnp.where(less, vectors[i][j], weights[i]) for i in range(order)]
    negative = weights[0] < 0.0
    weights = [jnp.where(negative, -w, w) for w in weights]
    return best * scale, weights


def kernel(
    dims,
    guess_ref,
    right_ref,
    blocks_ref,
    pairs_ref,
    left_hbm,
    vector_ref,
    residual_ref,
    left,
    mixing,
    right_rows,
    right_by_level,
    right_diag,
    gathered,
    column,
    inner,
    image,
    pair_out,
    pair_in,
    block_out,
    block_in,
    diag_parts,
    diag_in,
    basis,
    images,
    tile_out,
    tiles_a,
    tile_mid,
    tiles_b,
    final_out,
    final_in,
    guess_rows,
    left_sem,
    x_send,
    x_recv,
    f_send,
    f_recv,
    z_send,
    z_recv,
    c_send,
    c_recv,
    p_send,
    p_recv,
    s_send,
    s_recv,
    a_send,
    a_recv,
    b_send,
    b_recv,
    d_sems,
    o_sems,
):
    n_lb, n_rb, line, rows, states, window, levels, local_levels, count = dims
    lines = n_rb // line
    chunk = line * rows
    half_width = states * window // 2
    block_rows = n_lb * rows
    scale = 1.0 / (n_lb * n_rb * rows * states * window)
    z = lax.axis_index("lb")
    me = lax.axis_index("rb")
    half = lax.axis_index("wa")
    other = 1 - half
    my_line, my_place = lax.div(me, line), lax.rem(me, line)
    f32, bf16 = jnp.float32, jnp.bfloat16

    def remote(src, dst, send, recv, peer):
        return pltpu.make_async_remote_copy(
            src_ref=src, dst_ref=dst, send_sem=send, recv_sem=recv, device_id=peer, device_id_type=MESH_ID
        )

    def drain(region, sem):
        pltpu.make_async_copy(region, region, sem).wait()

    def each(count, body, unroll=False):
        def step(i, carry):
            body(i)
            return carry

        lax.fori_loop(0, count, step, 0, unroll=unroll)

    def left_copy(i):
        w, q = lax.div(i, lines), lax.rem(i, lines)
        return pltpu.make_async_copy(
            left_hbm.at[w, :, pl.ds(pl.multiple_of(q * chunk, chunk), chunk)],
            left.at[q, :, pl.ds(pl.multiple_of(w * chunk, chunk), chunk)],
            left_sem,
        )

    each(local_levels * lines, lambda i: left_copy(i).start())

    barrier = pltpu.get_barrier_semaphore()

    def greet(peer):
        pl.semaphore_signal(barrier, inc=1, device_id=peer, device_id_type=MESH_ID)

    each(n_rb - 1, lambda j: greet({"rb": lax.rem(me + 1 + j, n_rb)}))
    each(n_lb - 1, lambda j: greet({"lb": lax.rem(z + 1 + j, n_lb)}))
    each(n_lb, lambda j: greet({"lb": lax.rem(z + j, n_lb), "wa": other}))

    def block(it, side, x, y):
        return gathered.at[it, side, pl.ds(pl.multiple_of((x * line + y) * rows, rows), rows)]

    def send_block(it, x, y, to_x, to_y):
        region = block(it, half, x, y)
        peer = {"rb": lax.rem(to_x, lines) * line + lax.rem(to_y, line)}
        remote(region, region, x_send.at[it], x_recv.at[it, x * line + y], peer).start()

    def forward(it, x, y):
        region = block(it, half, x, y)
        remote(region, region, f_send.at[it], f_recv.at[it, x * line + y], {"wa": other}).start()

    def hand_out(it, part):
        block(it, half, my_line, my_place)[...] = part
        column[it, half, z] = part

    def far_first(j, size):
        step = lax.div(j + 1, 2)
        return size // 2 + step - 2 * step * lax.rem(j, 2)

    def start_hand_out(it):
        def to_axes(j):
            d = far_first(j, line)
            send_block(it, my_line, my_place, my_line, my_place + d)
            send_block(it, my_line, my_place, my_line + d, my_place)

        def to_column(j):
            region = column.at[it, half, z]
            remote(region, region, z_send.at[it], z_recv.at[it], {"lb": lax.rem(z + 1 + j, n_lb)}).start()

        each(line - 1, to_axes, True)
        forward(it, my_line, my_place)
        each(n_lb - 1, to_column)

    def pass_on(it):
        def one(j):
            d = j + 1 + j - 3 * lax.div(j, 2)
            on_x = 1 - lax.rem(my_line + my_place + d, 2)
            x, y = lax.rem(my_line + d * on_x, lines), lax.rem(my_place + d * (1 - on_x), line)
            drain(block(it, half, x, y), x_recv.at[it, x * line + y])

            def to(k):
                e = far_first(k, line)
                send_block(it, x, y, my_line + e * (1 - on_x), my_place + e * on_x)

            each(line - 1, to, True)
            forward(it, x, y)

        each(line - 1, one)

    def arrive(it, x):
        for y in range(line):
            same_x, same_y = x == my_line, my_place == y
            odd = lax.rem(x + y, 2) == 1
            done = (same_x & same_y) | (same_y & ~same_x & ~odd) | (same_x & ~same_y & odd)

            @pl.when(jnp.logical_not(done))
            def _():
                drain(block(it, half, x, y), x_recv.at[it, x * line + y])
                forward(it, x, y)

    for r in range(rows):
        guess_rows[r * states : (r + 1) * states, :] = guess_ref[r].astype(f32)
    first = jnp.concatenate(
        [
            guess_rows[pl.ds(half * (states // 2) + k, rows, stride=states), :].astype(bf16)
            for k in range(states // 2)
        ],
        axis=1,
    )
    hand_out(0, first)
    current = first.astype(f32)
    pl.semaphore_wait(barrier, (n_rb - 1) + (n_lb - 1) + n_lb)
    start_hand_out(0)

    right_rows[...] = right_ref[...].astype(f32).reshape(window * levels, window)
    for v in range(levels):
        right_by_level[v] = right_rows[pl.ds(v, window, stride=levels), :]

    def factor(n, w, t, s):
        named = jnp.where(pairs_ref[0, n] == half * local_levels + w, 0.5, 0.0)
        return named * (blocks_ref[t, s, n] + blocks_ref[s, t, n])

    def mix_level(w):
        for t in range(states):
            for s in range(t, states):

                def add_block(n, tile):
                    return tile + factor(n, w, t, s) * right_by_level[pairs_ref[1, n]]

                tile = lax.fori_loop(0, count, add_block, jnp.zeros((window, window), f32), unroll=4).astype(bf16)
                for a, b in {(t, s), (s, t)}:
                    mixing[w, a // 2, b * window : (b + 1) * window, (a % 2) * window : (a % 2 + 1) * window] = tile

    early = local_levels // 2
    each(early, mix_level)
    pass_on(0)
    each(local_levels - early, lambda w: mix_level(w + early))

    row_at = lax.broadcasted_iota(jnp.int32, (window, window), 0)
    col_at = lax.broadcasted_iota(jnp.int32, (window, window), 1)
    for v in range(levels):
        on_diagonal = jnp.where(row_at == col_at, right_by_level[v], 0.0)
        right_diag[v] = jnp.broadcast_to(jnp.sum(on_diagonal, axis=0, keepdims=True), TILE)
    each(local_levels * lines, lambda i: left_copy(i).wait())
    q_own = my_line
    inside = lax.rem(me, line) * rows
    at_row = lax.broadcasted_iota(jnp.int32, (rows, chunk), 0)
    at_col = lax.broadcasted_iota(jnp.int32, (rows, chunk), 1)
    picked = at_col == at_row + inside
    parts = [jnp.zeros((rows, window), f32) for _ in range(states)]
    for w in range(local_levels):
        entries = left[q_own, pl.ds(pl.multiple_of(z * rows, rows), rows), w * chunk : (w + 1) * chunk].astype(f32)
        left_diag = jnp.sum(jnp.where(picked, entries, 0.0), axis=1, keepdims=True)
        for s in range(states):
            along = lax.fori_loop(
                0, count, lambda n, a, s=s, w=w: a + factor(n, w, s, s) * right_diag[pairs_ref[1, n]], jnp.zeros(TILE, f32)
            )
            parts[s] = parts[s] + left_diag * along[0:1]
    for s in range(states):
        diag_parts[s // 2, :, (s % 2) * window : (s % 2 + 1) * window] = parts[s]
    diag_copy = remote(diag_parts.at[other], diag_in, d_sems.at[0], d_sems.at[1], {"wa": other})
    diag_copy.start()

    def spread(number):
        piece = jnp.concatenate([number] * (rows // TILE[0]), axis=0)
        return jnp.concatenate([piece] * (half_width // TILE[1]), axis=1)

    def fold(value):
        groups = jnp.sum(value.reshape(rows // TILE[0], TILE[0], half_width), axis=0)
        out = groups[:, : TILE[1]]
        for i in range(1, half_width // TILE[1]):
            out = out + groups[:, i * TILE[1] : (i + 1) * TILE[1]]
        return out

    def chunk_rows(q):
        return pl.ds(pl.multiple_of(q * chunk, chunk), chunk)

    def line_at(i):
        if lines == 4:
            i = i + lax.div(i, 2) - 2 * lax.div(i, 3)
        return lax.rem(my_line + i, lines)

    def forward_column(it):
        region = column.at[it, half]
        return remote(region, region, c_send.at[it], c_recv.at[it], {"wa": other})

    def multiply(it, q):
        x = jnp.concatenate([gathered[it, 0, chunk_rows(q), :], gathered[it, 1, chunk_rows(q), :]], axis=1)

        for h in range(2):
            for w in range(local_levels):
                inner[h, w * chunk : (w + 1) * chunk, :] = jnp.dot(
                    x, mixing[w, h], preferred_element_type=f32
                ).astype(bf16)
        for h in range(2):
            image[h] += jnp.dot(left[q], inner[h], preferred_element_type=f32)

    def row_sums(first_row, values):
        row = lax.broadcasted_iota(jnp.int32, TILE, 0)
        tile = jnp.zeros(TILE, f32)
        for i, value in enumerate(values):
            value = jnp.sum(value, axis=0, keepdims=True)
            tile = jnp.where(row == first_row + i, jnp.broadcast_to(value, TILE), tile)
        return tile

    def apply(it, member):
        if it > 0:
            pass_on(it)
        image[...] = jnp.zeros_like(image)
        sums = [fold(member * member)]
        sums += [fold(basis[j] * member) for j in range(it)]
        sums += [fold(images[j] * member) for j in range(it)]
        tile_out[it] = row_sums(1, sums)
        arrive(it, my_line)
        pair = remote(pair_out.at[it], pair_in.at[it], p_send.at[it], p_recv.at[it], {"wa": other})

        def one_line(i):
            @pl.when(i == lines - 1)
            def _():
                drain(column.at[it, half, pl.ds(0, n_lb - 1)], z_recv.at[it])
                forward_column(it).start()

            q = line_at(i)
            for y in range(line):
                drain(block(it, other, q, y), f_recv.at[it, q * line + y])
            multiply(it, q)

            @pl.when(i == 0)
            def _():
                arrive(it, line_at(1))

            @pl.when(i < lines - 2)
            def _():
                arrive(it, line_at(i + 2))

        each(lines, one_line)
        pair_out[it] = image[other].astype(bf16)
        pair.start()
        drain(column.at[it, other], c_recv.at[it])
        product = jnp.zeros(TILE, f32)
        for h in range(2):
            for b in range(n_lb):
                product = product + fold(image[h, b * rows : (b + 1) * rows, :] * column[it, h, b].astype(f32))
        tile = tile_out[it] + row_sums(0, [product])

        def to_block(j):
            b = lax.rem(z + far_first(j, n_lb), n_lb)
            remote(block_out.at[it, b], block_in.at[it, z], s_send.at[it], s_recv.at[it], {"lb": b}).start()

        def exchange_blocks():
            pair.wait_recv()
            summed = image[half] + pair_in[it].astype(f32)
            image[half] = summed
            block_out[it] = summed.astype(bf16).reshape(n_lb, rows, half_width)
            each(n_lb - 1, to_block, True)

        def collect():
            drain(block_in.at[it, pl.ds(0, n_lb - 1)], s_recv.at[it])
            total = image[half, pl.ds(pl.multiple_of(z * rows, rows), rows), :]
            for j in range(1, n_lb):
                total = total + block_in[it, lax.rem(z + j, n_lb)].astype(f32)
            return total

        return add_up(it, tile, exchange_blocks), collect

    def add_up(it, tile, between):
        slot = z * 2 + half
        tile_out[it] = tile

        def to_column(j):
            peer = {"lb": lax.rem(z + 1 + j, n_lb), "wa": 1}
            remote(tile_out.at[it], tiles_a.at[it, slot], a_send.at[it], a_recv.at[it], peer).start()

        each(n_lb - 1, to_column, True)

        @pl.when(half == 0)
        def _():
            remote(tile_out.at[it], tiles_a.at[it, slot], a_send.at[it], a_recv.at[it], {"wa": 1}).start()

        @pl.when(half == 1)
        def _():
            tiles_a[it, slot] = tile

        between()

        @pl.when(half == 1)
        def _():
            drain(tiles_a.at[it, pl.ds(0, 2 * n_lb - 1)], a_recv.at[it])
            summed = tiles_a[it, 0]
            for j in range(1, 2 * n_lb):
                summed = summed + tiles_a[it, j]
            tile_mid[it] = summed
            tiles_b[it, me] = summed

            def to_plane(j):
                peer = {"rb": lax.rem(me + lax.div(j + 1, 2), n_rb), "wa": lax.rem(j, 2)}
                remote(tile_mid.at[it], tiles_b.at[it, me], b_send.at[it], b_recv.at[it], peer).start()

            each(2 * n_rb - 1, to_plane, True)
            drain(tiles_b.at[it, pl.ds(0, n_rb - 1)], b_recv.at[it])

        @pl.when(half == 0)
        def _():
            drain(tiles_b.at[it], b_recv.at[it])

        tile = tiles_b[it, 0]
        for j in range(1, n_rb):
            tile = tile + tiles_b[it, j]
        tile = jnp.broadcast_to(jnp.sum(tile, axis=1, keepdims=True), TILE) * scale
        return [jnp.broadcast_to(tile[i : i + 1, :], TILE) for i in range(2 + 2 * it)]

    entries = [[None] * STEPS for _ in range(STEPS)]
    diagonal = None
    for it in range(STEPS):
        totals, collect = apply(it, current)
        energy, square = totals[0], totals[1]
        overlaps, crossed = totals[2 : 2 + it], totals[2 + it :]
        norm = square
        for a in overlaps:
            norm = norm - a * a
        inverse = lax.rsqrt(jnp.maximum(norm, 0.0) + epsilon)
        for j in range(it):
            value = crossed[j]
            for i in range(it):
                value = value - overlaps[i] * entries[i][j]
            entries[j][it] = entries[it][j] = inverse * value
            energy = energy - overlaps[j] * (crossed[j] + value)
        entries[it][it] = inverse * inverse * energy
        theta, weights = lowest(entries, it + 1)

        vector, applied_now = current, collect()
        for j in range(it):
            a = spread(overlaps[j])
            vector = vector - a * basis[j]
            applied_now = applied_now - a * images[j]
        grow = spread(inverse)
        vector, applied_now = vector * grow, applied_now * grow
        basis[it] = vector
        images[it] = applied_now
        last = spread(weights[it])
        ritz, residual = last * vector, last * applied_now
        for j in range(it):
            a = spread(weights[j])
            ritz = ritz + a * basis[j]
            residual = residual + a * images[j]
        shift = spread(theta)
        residual = residual - shift * ritz
        if it == 0:
            diag_copy.wait()
            diagonal = diag_parts[half] + diag_in[...]
            diag_parts[half] = diagonal
        if it < ITERS:
            current = residual / (jnp.abs(diag_parts[half] - shift) + 1.0)
            hand_out(it + 1, current.astype(bf16))
            start_hand_out(it + 1)

    outputs = (vector_ref, residual_ref)
    for i, value in enumerate((ritz, residual)):
        final_out[i] = value
    last_copy = remote(final_out, final_in, o_sems.at[0], o_sems.at[1], {"wa": other})
    last_copy.start()

    def put(i, side, value):
        for k in range(states // 2):
            outputs[i][pl.ds(side * (states // 2) + k, rows, stride=states), :] = value[:, k * window : (k + 1) * window]

    for side in range(2):

        @pl.when(half == side)
        def _():
            for i, value in enumerate((ritz, residual)):
                put(i, side, value)

    def finish(it):
        drain(gathered.at[it, 0, pl.ds(0, (n_rb - 1) * rows)], x_send.at[it])
        drain(column.at[it, half, pl.ds(0, n_lb - 1)], z_send.at[it])
        forward_column(it).wait_send()
        drain(gathered.at[it, half], f_send.at[it])
        drain(pair_out.at[it], p_send.at[it])
        drain(block_out.at[it, pl.ds(0, n_lb - 1)], s_send.at[it])
        drain(tiles_a.at[it, pl.ds(0, n_lb - 1)], a_send.at[it])

        @pl.when(half == 0)
        def _():
            drain(tiles_a.at[it, 0], a_send.at[it])

        @pl.when(half == 1)
        def _():
            drain(tiles_b.at[it], b_send.at[it])
            drain(tiles_b.at[it, pl.ds(0, n_rb - 1)], b_send.at[it])

    each(STEPS, finish)
    last_copy.wait()
    for side in range(2):

        @pl.when(half == 1 - side)
        def _():
            for i in range(2):
                put(i, side, final_in[i])


def per_device(initial_guess, left_environment, right_environment, operator_blocks, operator_pairs):
    rows, states, window = initial_guess.shape
    levels = right_environment.shape[1]
    local_levels, n_lb = left_environment.shape[:2]
    contracted = left_environment.shape[4]
    n_rb = lax.axis_size("rb")
    line = 4 if n_rb == 16 else 2
    lines, chunk = n_rb // line, line * rows
    width, half_width = states * window, states * window // 2
    block_rows = n_lb * rows
    dims = (n_lb, n_rb, line, rows, states, window, levels, local_levels, operator_pairs.shape[0])
    f32, bf16 = jnp.float32, jnp.bfloat16
    dma = pltpu.SemaphoreType.DMA
    vmem = pl.BlockSpec(memory_space=pltpu.VMEM)
    smem = pl.BlockSpec(memory_space=pltpu.SMEM)
    out = jax.ShapeDtypeStruct((rows * states, window), f32)
    outs = pl.pallas_call(
        functools.partial(kernel, dims),
        out_shape=(out, out),
        in_specs=[vmem, vmem, smem, smem, pl.BlockSpec(memory_space=pltpu.HBM)],
        out_specs=(vmem, vmem),
        scratch_shapes=[
            pltpu.VMEM((lines, block_rows, local_levels * chunk), bf16),
            pltpu.VMEM((local_levels, 2, width, half_width), bf16),
            pltpu.VMEM((window * levels, window), f32),
            pltpu.VMEM((levels, window, window), f32),
            pltpu.VMEM((levels, *TILE), f32),
            pltpu.VMEM((STEPS, 2, contracted, half_width), bf16),
            pltpu.VMEM((STEPS, 2, n_lb, rows, half_width), bf16),
            pltpu.VMEM((2, local_levels * chunk, half_width), bf16),
            pltpu.VMEM((2, block_rows, half_width), f32),
            pltpu.VMEM((STEPS, block_rows, half_width), bf16),
            pltpu.VMEM((STEPS, block_rows, half_width), bf16),
            pltpu.VMEM((STEPS, n_lb, rows, half_width), bf16),
            pltpu.VMEM((STEPS, n_lb, rows, half_width), bf16),
            pltpu.VMEM((2, rows, half_width), f32),
            pltpu.VMEM((rows, half_width), f32),
            pltpu.VMEM((STEPS, rows, half_width), f32),
            pltpu.VMEM((STEPS, rows, half_width), f32),
            pltpu.VMEM((STEPS, *TILE), f32),
            pltpu.VMEM((STEPS, 2 * n_lb, *TILE), f32),
            pltpu.VMEM((STEPS, *TILE), f32),
            pltpu.VMEM((STEPS, n_rb, *TILE), f32),
            pltpu.VMEM((2, rows, half_width), f32),
            pltpu.VMEM((2, rows, half_width), f32),
            pltpu.VMEM((rows * states, window), f32),
            dma(()),
            dma((STEPS,)),
            dma((STEPS, n_rb)),
            dma((STEPS,)),
            dma((STEPS, n_rb)),
            dma((STEPS,)),
            dma((STEPS,)),
            dma((STEPS,)),
            dma((STEPS,)),
            dma((STEPS,)),
            dma((STEPS,)),
            dma((STEPS,)),
            dma((STEPS,)),
            dma((STEPS,)),
            dma((STEPS,)),
            dma((STEPS,)),
            dma((STEPS,)),
            dma((2,)),
            dma((2,)),
        ],
        compiler_params=pltpu.CompilerParams(collective_id=0, has_side_effects=True),
        name="davidson",
    )(
        initial_guess,
        right_environment,
        operator_blocks.transpose(1, 2, 0),
        operator_pairs.T,
        left_environment.reshape(local_levels, block_rows, contracted),
    )
    return tuple(o.reshape(rows, states, window) for o in outs)


def solution(mesh):
    in_specs = (P(LB_RB, None, None), P("wa", None, "rb", None, "lb"), P(), P(), P())
    out_specs = (P(LB_RB, None, None), P(LB_RB, None, None))
    return jax.shard_map(per_device, mesh=mesh, in_specs=in_specs, out_specs=out_specs, check_vma=False)
```

```python
import functools

import jax
import jax.numpy as jnp
from jax import lax
from jax.experimental import pallas as pl
from jax.experimental.pallas import tpu as pltpu
from jax.sharding import PartitionSpec as P

ITERS = 3
SWEEPS = 8
STEPS = ITERS + 1
TILE = (8, 128)
LB_RB = ("lb", "rb")
MESH_ID = pl.DeviceIdType.MESH

highest = lax.Precision.HIGHEST
epsilon = 1e-06


def rotate(matrix, vectors, p, q, order):
    y = 2.0 * matrix[p][q]
    x = matrix[q][q] - matrix[p][p]
    square = x * x + y * y
    usable = square > 0.0
    inverse = lax.rsqrt(jnp.where(usable, square, 1.0))
    half_sum = 0.5 + 0.5 * jnp.abs(x * inverse)
    inverse_large = lax.rsqrt(half_sum)
    large = half_sum * inverse_large
    small = 0.5 * jnp.abs(y * inverse) * inverse_large
    forward = x >= 0.0
    cosine = jnp.where(usable, jnp.where(forward, large, small), 1.0)
    sine = jnp.where(usable, jnp.where(forward, small, large), 0.0)
    sine = jnp.where(y < 0.0, -sine, sine)
    m_pp, m_qq, m_pq = matrix[p][p], matrix[q][q], matrix[p][q]
    cc, ss, cs = cosine * cosine, sine * sine, cosine * sine
    cross = 2.0 * cs * m_pq
    matrix[p][p] = cc * m_pp - cross + ss * m_qq
    matrix[q][q] = ss * m_pp + cross + cc * m_qq
    matrix[p][q] = matrix[q][p] = jnp.zeros_like(m_pq)
    for i in range(order):
        if i != p and i != q:
            a, b = matrix[i][p], matrix[i][q]
            matrix[i][p] = matrix[p][i] = cosine * a - sine * b
            matrix[i][q] = matrix[q][i] = sine * a + cosine * b
        a, b = vectors[i][p], vectors[i][q]
        vectors[i][p] = cosine * a - sine * b
        vectors[i][q] = sine * a + cosine * b


def lowest(entries, order):
    if order == 1:
        return entries[0][0], [jnp.ones(TILE, jnp.float32)]
    scale = jnp.abs(entries[0][0])
    for i in range(order):
        for j in range(i, order):
            scale = jnp.maximum(scale, jnp.abs(entries[i][j]))
    inverse = 1.0 / jnp.where(scale > 0.0, scale, 1.0)
    flat = [entries[i][j] * inverse for i in range(order) for j in range(order)]
    flat += [jnp.full(TILE, 1.0 if i == j else 0.0, jnp.float32) for i in range(order) for j in range(order)]

    def sweep(_, flat):
        matrix = [list(flat[i * order : (i + 1) * order]) for i in range(order)]
        base = order * order
        vectors = [list(flat[base + i * order : base + (i + 1) * order]) for i in range(order)]
        for p in range(order):
            for q in range(p + 1, order):
                rotate(matrix, vectors, p, q, order)
        return tuple(v for row in matrix + vectors for v in row)

    flat = lax.fori_loop(0, 1 if order == 2 else SWEEPS, sweep, tuple(flat))
    matrix = [flat[i * order : (i + 1) * order] for i in range(order)]
    base = order * order
    vectors = [flat[base + i * order : base + (i + 1) * order] for i in range(order)]
    best = matrix[0][0]
    weights = [vectors[i][0] for i in range(order)]
    for j in range(1, order):
        less = matrix[j][j] < best
        best = jnp.where(less, matrix[j][j], best)
        weights = [jnp.where(less, vectors[i][j], weights[i]) for i in range(order)]
    negative = weights[0] < 0.0
    weights = [jnp.where(negative, -w, w) for w in weights]
    return best * scale, weights


def kernel(
    dims,
    guess_ref,
    right_ref,
    blocks_ref,
    pairs_ref,
    left_hbm,
    vector_ref,
    residual_ref,
    left,
    mixing,
    right_rows,
    right_by_level,
    right_diag,
    gathered,
    column,
    inner,
    image,
    pair_out,
    pair_in,
    block_out,
    block_in,
    diag_parts,
    diag_in,
    basis,
    images,
    tile_out,
    tiles_a,
    tile_mid,
    tiles_b,
    final_out,
    final_in,
    guess_rows,
    left_sem,
    x_send,
    x_recv,
    f_send,
    f_recv,
    z_send,
    z_recv,
    c_send,
    c_recv,
    p_send,
    p_recv,
    s_send,
    s_recv,
    a_send,
    a_recv,
    b_send,
    b_recv,
    d_sems,
    o_sems,
):
    n_lb, n_rb, line, rows, states, window, levels, local_levels, count = dims
    lines = n_rb // line
    chunk = line * rows
    half_width = states * window // 2
    block_rows = n_lb * rows
    scale = 1.0 / (n_lb * n_rb * rows * states * window)
    z = lax.axis_index("lb")
    me = lax.axis_index("rb")
    half = lax.axis_index("wa")
    other = 1 - half
    my_line, my_place = lax.div(me, line), lax.rem(me, line)
    f32, bf16 = jnp.float32, jnp.bfloat16

    def remote(src, dst, send, recv, peer):
        return pltpu.make_async_remote_copy(
            src_ref=src, dst_ref=dst, send_sem=send, recv_sem=recv, device_id=peer, device_id_type=MESH_ID
        )

    def drain(region, sem):
        pltpu.make_async_copy(region, region, sem).wait()

    def each(count, body, unroll=False):
        def step(i, carry):
            body(i)
            return carry

        lax.fori_loop(0, count, step, 0, unroll=unroll)

    def left_copy(i):
        w, q = lax.div(i, lines), lax.rem(i, lines)
        return pltpu.make_async_copy(
            left_hbm.at[w, :, pl.ds(pl.multiple_of(q * chunk, chunk), chunk)],
            left.at[q, :, pl.ds(pl.multiple_of(w * chunk, chunk), chunk)],
            left_sem,
        )

    each(local_levels * lines, lambda i: left_copy(i).start())

    barrier = pltpu.get_barrier_semaphore()

    def greet(peer):
        pl.semaphore_signal(barrier, inc=1, device_id=peer, device_id_type=MESH_ID)

    each(n_rb - 1, lambda j: greet({"rb": lax.rem(me + 1 + j, n_rb)}))
    each(n_lb - 1, lambda j: greet({"lb": lax.rem(z + 1 + j, n_lb)}))
    each(n_lb, lambda j: greet({"lb": lax.rem(z + j, n_lb), "wa": other}))

    def block(it, side, x, y):
        return gathered.at[it, side, pl.ds(pl.multiple_of((x * line + y) * rows, rows), rows)]

    def send_block(it, x, y, to_x, to_y):
        region = block(it, half, x, y)
        peer = {"rb": lax.rem(to_x, lines) * line + lax.rem(to_y, line)}
        remote(region, region, x_send.at[it], x_recv.at[it, x * line + y], peer).start()

    def forward(it, x, y):
        region = block(it, half, x, y)
        remote(region, region, f_send.at[it], f_recv.at[it, x * line + y], {"wa": other}).start()

    def hand_out(it, part):
        block(it, half, my_line, my_place)[...] = part
        column[it, half, z] = part

    def far_first(j, size):
        step = lax.div(j + 1, 2)
        return size // 2 + step - 2 * step * lax.rem(j, 2)

    def start_hand_out(it):
        def to_axes(j):
            d = far_first(j, line)
            send_block(it, my_line, my_place, my_line, my_place + d)
            send_block(it, my_line, my_place, my_line + d, my_place)

        def to_column(j):
            region = column.at[it, half, z]
            remote(region, region, z_send.at[it], z_recv.at[it], {"lb": lax.rem(z + 1 + j, n_lb)}).start()

        each(line - 1, to_axes, True)
        forward(it, my_line, my_place)
        each(n_lb - 1, to_column)

    def pass_on(it):
        def one(j):
            d = j + 1 + j - 3 * lax.div(j, 2)
            on_x = 1 - lax.rem(my_line + my_place + d, 2)
            x, y = lax.rem(my_line + d * on_x, lines), lax.rem(my_place + d * (1 - on_x), line)
            drain(block(it, half, x, y), x_recv.at[it, x * line + y])

            def to(k):
                e = far_first(k, line)
                send_block(it, x, y, my_line + e * (1 - on_x), my_place + e * on_x)

            each(line - 1, to, True)
            forward(it, x, y)

        each(line - 1, one)

    def arrive(it, x):
        for y in range(line):
            same_x, same_y = x == my_line, my_place == y
            odd = lax.rem(x + y, 2) == 1
            done = (same_x & same_y) | (same_y & ~same_x & ~odd) | (same_x & ~same_y & odd)

            @pl.when(jnp.logical_not(done))
            def _():
                drain(block(it, half, x, y), x_recv.at[it, x * line + y])
                forward(it, x, y)

    for r in range(rows):
        guess_rows[r * states : (r + 1) * states, :] = guess_ref[r].astype(f32)
    first = jnp.concatenate(
        [
            guess_rows[pl.ds(half * (states // 2) + k, rows, stride=states), :].astype(bf16)
            for k in range(states // 2)
        ],
        axis=1,
    )
    hand_out(0, first)
    current = first.astype(f32)
    pl.semaphore_wait(barrier, (n_rb - 1) + (n_lb - 1) + n_lb)
    start_hand_out(0)

    right_rows[...] = right_ref[...].astype(f32).reshape(window * levels, window)
    for v in range(levels):
        right_by_level[v] = right_rows[pl.ds(v, window, stride=levels), :]

    def factor(n, w, t, s):
        named = jnp.where(pairs_ref[0, n] == half * local_levels + w, 0.5, 0.0)
        return named * (blocks_ref[t, s, n] + blocks_ref[s, t, n])

    def mix_level(w):
        for t in range(states):
            for s in range(t, states):

                def add_block(n, tile):
                    return tile + factor(n, w, t, s) * right_by_level[pairs_ref[1, n]]

                tile = lax.fori_loop(0, count, add_block, jnp.zeros((window, window), f32), unroll=4).astype(bf16)
                for a, b in {(t, s), (s, t)}:
                    mixing[w, a // 2, b * window : (b + 1) * window, (a % 2) * window : (a % 2 + 1) * window] = tile

    early = 1
    each(early, mix_level)
    pass_on(0)
    each(local_levels - early, lambda w: mix_level(w + early))

    row_at = lax.broadcasted_iota(jnp.int32, (window, window), 0)
    col_at = lax.broadcasted_iota(jnp.int32, (window, window), 1)
    for v in range(levels):
        on_diagonal = jnp.where(row_at == col_at, right_by_level[v], 0.0)
        right_diag[v] = jnp.broadcast_to(jnp.sum(on_diagonal, axis=0, keepdims=True), TILE)
    each(local_levels * lines, lambda i: left_copy(i).wait())
    q_own = my_line
    inside = lax.rem(me, line) * rows
    at_row = lax.broadcasted_iota(jnp.int32, (rows, chunk), 0)
    at_col = lax.broadcasted_iota(jnp.int32, (rows, chunk), 1)
    picked = at_col == at_row + inside
    parts = [jnp.zeros((rows, window), f32) for _ in range(states)]
    for w in range(local_levels):
        entries = left[q_own, pl.ds(pl.multiple_of(z * rows, rows), rows), w * chunk : (w + 1) * chunk].astype(f32)
        left_diag = jnp.sum(jnp.where(picked, entries, 0.0), axis=1, keepdims=True)
        for s in range(states):
            along = lax.fori_loop(
                0, count, lambda n, a, s=s, w=w: a + factor(n, w, s, s) * right_diag[pairs_ref[1, n]], jnp.zeros(TILE, f32)
            )
            parts[s] = parts[s] + left_diag * along[0:1]
    for s in range(states):
        diag_parts[s // 2, :, (s % 2) * window : (s % 2 + 1) * window] = parts[s]
    diag_copy = remote(diag_parts.at[other], diag_in, d_sems.at[0], d_sems.at[1], {"wa": other})
    diag_copy.start()

    def spread(number):
        piece = jnp.concatenate([number] * (rows // TILE[0]), axis=0)
        return jnp.concatenate([piece] * (half_width // TILE[1]), axis=1)

    def fold(value):
        groups = jnp.sum(value.reshape(rows // TILE[0], TILE[0], half_width), axis=0)
        out = groups[:, : TILE[1]]
        for i in range(1, half_width // TILE[1]):
            out = out + groups[:, i * TILE[1] : (i + 1) * TILE[1]]
        return out

    def chunk_rows(q):
        return pl.ds(pl.multiple_of(q * chunk, chunk), chunk)

    def line_at(i):
        if lines == 4:
            i = i + lax.div(i, 2) - 2 * lax.div(i, 3)
        return lax.rem(my_line + i, lines)

    def forward_column(it):
        region = column.at[it, half]
        return remote(region, region, c_send.at[it], c_recv.at[it], {"wa": other})

    def multiply(it, q):
        x = jnp.concatenate([gathered[it, 0, chunk_rows(q), :], gathered[it, 1, chunk_rows(q), :]], axis=1)

        for h in range(2):
            for w in range(local_levels):
                inner[h, w * chunk : (w + 1) * chunk, :] = jnp.dot(
                    x, mixing[w, h], preferred_element_type=f32
                ).astype(bf16)
        for h in range(2):
            image[h] += jnp.dot(left[q], inner[h], preferred_element_type=f32)

    def row_sums(first_row, values):
        row = lax.broadcasted_iota(jnp.int32, TILE, 0)
        tile = jnp.zeros(TILE, f32)
        for i, value in enumerate(values):
            value = jnp.sum(value, axis=0, keepdims=True)
            tile = jnp.where(row == first_row + i, jnp.broadcast_to(value, TILE), tile)
        return tile

    def apply(it, member):
        if it > 0:
            pass_on(it)
        image[...] = jnp.zeros_like(image)
        sums = [fold(member * member)]
        sums += [fold(basis[j] * member) for j in range(it)]
        sums += [fold(images[j] * member) for j in range(it)]
        tile_out[it] = row_sums(1, sums)
        arrive(it, my_line)
        pair = remote(pair_out.at[it], pair_in.at[it], p_send.at[it], p_recv.at[it], {"wa": other})

        def one_line(i):
            @pl.when(i == lines - 1)
            def _():
                drain(column.at[it, half, pl.ds(0, n_lb - 1)], z_recv.at[it])
                forward_column(it).start()

            q = line_at(i)
            for y in range(line):
                drain(block(it, other, q, y), f_recv.at[it, q * line + y])
            multiply(it, q)

            @pl.when(i == 0)
            def _():
                arrive(it, line_at(1))

            @pl.when(i < lines - 2)
            def _():
                arrive(it, line_at(i + 2))

        each(lines, one_line)
        pair_out[it] = image[other].astype(bf16)
        pair.start()
        drain(column.at[it, other], c_recv.at[it])
        product = jnp.zeros(TILE, f32)
        for h in range(2):
            for b in range(n_lb):
                product = product + fold(image[h, b * rows : (b + 1) * rows, :] * column[it, h, b].astype(f32))
        tile = tile_out[it] + row_sums(0, [product])

        def to_block(j):
            b = lax.rem(z + far_first(j, n_lb), n_lb)
            remote(block_out.at[it, b], block_in.at[it, z], s_send.at[it], s_recv.at[it], {"lb": b}).start()

        def exchange_blocks():
            pair.wait_recv()
            summed = image[half] + pair_in[it].astype(f32)
            image[half] = summed
            block_out[it] = summed.astype(bf16).reshape(n_lb, rows, half_width)
            each(n_lb - 1, to_block, True)

        def collect():
            drain(block_in.at[it, pl.ds(0, n_lb - 1)], s_recv.at[it])
            total = image[half, pl.ds(pl.multiple_of(z * rows, rows), rows), :]
            for j in range(1, n_lb):
                total = total + block_in[it, lax.rem(z + j, n_lb)].astype(f32)
            return total

        return add_up(it, tile, exchange_blocks), collect

    def add_up(it, tile, between):
        slot = z * 2 + half
        tile_out[it] = tile

        def to_column(j):
            peer = {"lb": lax.rem(z + 1 + j, n_lb), "wa": 1}
            remote(tile_out.at[it], tiles_a.at[it, slot], a_send.at[it], a_recv.at[it], peer).start()

        each(n_lb - 1, to_column, True)

        @pl.when(half == 0)
        def _():
            remote(tile_out.at[it], tiles_a.at[it, slot], a_send.at[it], a_recv.at[it], {"wa": 1}).start()

        @pl.when(half == 1)
        def _():
            tiles_a[it, slot] = tile

        between()

        @pl.when(half == 1)
        def _():
            drain(tiles_a.at[it, pl.ds(0, 2 * n_lb - 1)], a_recv.at[it])
            summed = tiles_a[it, 0]
            for j in range(1, 2 * n_lb):
                summed = summed + tiles_a[it, j]
            tile_mid[it] = summed
            tiles_b[it, me] = summed

            def to_plane(j):
                peer = {"rb": lax.rem(me + lax.div(j + 1, 2), n_rb), "wa": lax.rem(j, 2)}
                remote(tile_mid.at[it], tiles_b.at[it, me], b_send.at[it], b_recv.at[it], peer).start()

            each(2 * n_rb - 1, to_plane, True)
            drain(tiles_b.at[it, pl.ds(0, n_rb - 1)], b_recv.at[it])

        @pl.when(half == 0)
        def _():
            drain(tiles_b.at[it], b_recv.at[it])

        tile = tiles_b[it, 0]
        for j in range(1, n_rb):
            tile = tile + tiles_b[it, j]
        tile = jnp.broadcast_to(jnp.sum(tile, axis=1, keepdims=True), TILE) * scale
        return [jnp.broadcast_to(tile[i : i + 1, :], TILE) for i in range(2 + 2 * it)]

    entries = [[None] * STEPS for _ in range(STEPS)]
    diagonal = None
    for it in range(STEPS):
        totals, collect = apply(it, current)
        energy, square = totals[0], totals[1]
        overlaps, crossed = totals[2 : 2 + it], totals[2 + it :]
        norm = square
        for a in overlaps:
            norm = norm - a * a
        inverse = lax.rsqrt(jnp.maximum(norm, 0.0) + epsilon)
        for j in range(it):
            value = crossed[j]
            for i in range(it):
                value = value - overlaps[i] * entries[i][j]
            entries[j][it] = entries[it][j] = inverse * value
            energy = energy - overlaps[j] * (crossed[j] + value)
        entries[it][it] = inverse * inverse * energy
        theta, weights = lowest(entries, it + 1)

        vector, applied_now = current, collect()
        for j in range(it):
            a = spread(overlaps[j])
            vector = vector - a * basis[j]
            applied_now = applied_now - a * images[j]
        grow = spread(inverse)
        vector, applied_now = vector * grow, applied_now * grow
        last = spread(weights[it])
        ritz, residual = last * vector, last * applied_now
        for j in range(it):
            a = spread(weights[j])
            ritz = ritz + a * basis[j]
            residual = residual + a * images[j]
        shift = spread(theta)
        residual = residual - shift * ritz
        if it == 0:
            diag_copy.wait()
            diagonal = diag_parts[half] + diag_in[...]
            diag_parts[half] = diagonal
        if it < ITERS:
            current = residual / (jnp.abs(diag_parts[half] - shift) + 1.0)
            hand_out(it + 1, current.astype(bf16))
            start_hand_out(it + 1)
            basis[it] = vector
            images[it] = applied_now

    outputs = (vector_ref, residual_ref)
    for i, value in enumerate((ritz, residual)):
        final_out[i] = value
    last_copy = remote(final_out, final_in, o_sems.at[0], o_sems.at[1], {"wa": other})
    last_copy.start()

    def put(i, side, value):
        for k in range(states // 2):
            outputs[i][pl.ds(side * (states // 2) + k, rows, stride=states), :] = value[:, k * window : (k + 1) * window]

    for side in range(2):

        @pl.when(half == side)
        def _():
            for i, value in enumerate((ritz, residual)):
                put(i, side, value)

    def finish(it):
        drain(gathered.at[it, 0, pl.ds(0, (n_rb - 1) * rows)], x_send.at[it])
        drain(column.at[it, half, pl.ds(0, n_lb - 1)], z_send.at[it])
        forward_column(it).wait_send()
        drain(gathered.at[it, half], f_send.at[it])
        drain(pair_out.at[it], p_send.at[it])
        drain(block_out.at[it, pl.ds(0, n_lb - 1)], s_send.at[it])
        drain(tiles_a.at[it, pl.ds(0, n_lb - 1)], a_send.at[it])

        @pl.when(half == 0)
        def _():
            drain(tiles_a.at[it, 0], a_send.at[it])

        @pl.when(half == 1)
        def _():
            drain(tiles_b.at[it], b_send.at[it])
            drain(tiles_b.at[it, pl.ds(0, n_rb - 1)], b_send.at[it])

    each(STEPS, finish)
    last_copy.wait()
    for side in range(2):

        @pl.when(half == 1 - side)
        def _():
            for i in range(2):
                put(i, side, final_in[i])


def per_device(initial_guess, left_environment, right_environment, operator_blocks, operator_pairs):
    rows, states, window = initial_guess.shape
    levels = right_environment.shape[1]
    local_levels, n_lb = left_environment.shape[:2]
    contracted = left_environment.shape[4]
    n_rb = lax.axis_size("rb")
    line = 4 if n_rb == 16 else 2
    lines, chunk = n_rb // line, line * rows
    width, half_width = states * window, states * window // 2
    block_rows = n_lb * rows
    dims = (n_lb, n_rb, line, rows, states, window, levels, local_levels, operator_pairs.shape[0])
    f32, bf16 = jnp.float32, jnp.bfloat16
    dma = pltpu.SemaphoreType.DMA
    vmem = pl.BlockSpec(memory_space=pltpu.VMEM)
    smem = pl.BlockSpec(memory_space=pltpu.SMEM)
    out = jax.ShapeDtypeStruct((rows * states, window), f32)
    outs = pl.pallas_call(
        functools.partial(kernel, dims),
        out_shape=(out, out),
        in_specs=[vmem, vmem, smem, smem, pl.BlockSpec(memory_space=pltpu.HBM)],
        out_specs=(vmem, vmem),
        scratch_shapes=[
            pltpu.VMEM((lines, block_rows, local_levels * chunk), bf16),
            pltpu.VMEM((local_levels, 2, width, half_width), bf16),
            pltpu.VMEM((window * levels, window), f32),
            pltpu.VMEM((levels, window, window), f32),
            pltpu.VMEM((levels, *TILE), f32),
            pltpu.VMEM((STEPS, 2, contracted, half_width), bf16),
            pltpu.VMEM((STEPS, 2, n_lb, rows, half_width), bf16),
            pltpu.VMEM((2, local_levels * chunk, half_width), bf16),
            pltpu.VMEM((2, block_rows, half_width), f32),
            pltpu.VMEM((STEPS, block_rows, half_width), bf16),
            pltpu.VMEM((STEPS, block_rows, half_width), bf16),
            pltpu.VMEM((STEPS, n_lb, rows, half_width), bf16),
            pltpu.VMEM((STEPS, n_lb, rows, half_width), bf16),
            pltpu.VMEM((2, rows, half_width), f32),
            pltpu.VMEM((rows, half_width), f32),
            pltpu.VMEM((STEPS, rows, half_width), f32),
            pltpu.VMEM((STEPS, rows, half_width), f32),
            pltpu.VMEM((STEPS, *TILE), f32),
            pltpu.VMEM((STEPS, 2 * n_lb, *TILE), f32),
            pltpu.VMEM((STEPS, *TILE), f32),
            pltpu.VMEM((STEPS, n_rb, *TILE), f32),
            pltpu.VMEM((2, rows, half_width), f32),
            pltpu.VMEM((2, rows, half_width), f32),
            pltpu.VMEM((rows * states, window), f32),
            dma(()),
            dma((STEPS,)),
            dma((STEPS, n_rb)),
            dma((STEPS,)),
            dma((STEPS, n_rb)),
            dma((STEPS,)),
            dma((STEPS,)),
            dma((STEPS,)),
            dma((STEPS,)),
            dma((STEPS,)),
            dma((STEPS,)),
            dma((STEPS,)),
            dma((STEPS,)),
            dma((STEPS,)),
            dma((STEPS,)),
            dma((STEPS,)),
            dma((STEPS,)),
            dma((2,)),
            dma((2,)),
        ],
        compiler_params=pltpu.CompilerParams(collective_id=0, has_side_effects=True),
        name="davidson",
    )(
        initial_guess,
        right_environment,
        operator_blocks.transpose(1, 2, 0),
        operator_pairs.T,
        left_environment.reshape(local_levels, block_rows, contracted),
    )
    return tuple(o.reshape(rows, states, window) for o in outs)


def solution(mesh):
    in_specs = (P(LB_RB, None, None), P("wa", None, "rb", None, "lb"), P(), P(), P())
    out_specs = (P(LB_RB, None, None), P(LB_RB, None, None))
    return jax.shard_map(per_device, mesh=mesh, in_specs=in_specs, out_specs=out_specs, check_vma=False)
```
